32 devices in a mesh: dp: 4 (over y, x), expert: 8 (over z, core).
Axes of the slice: x: 2, y: 2, z: 4, core: 2. Of those that a mesh axis runs over, the one named last changes fastest.
Arguments:
- tokens: bfloat16 [1024, 4096], P('dp', 'expert'), may hold values from -6 to 6
- routing: int32 [1024, 2], P('dp'), may hold values from 0 to 3, all different within a row; in each aligned block of 256 rows (0 to 255, 256 to 511, ...) at most 192 rows name the same one
- gate_weight: bfloat16 [4096, 4], P('expert'), may hold values from -0.09375 to 0.09375
- expert_in: bfloat16 [4, 4096, 8192], P('dp', None, 'expert'), may hold values from -0.09375 to 0.09375
- expert_out: bfloat16 [4, 8192, 4096], P('dp', 'expert'), may hold values from -0.75 to 0.75
Outputs:
- mixed: bfloat16 [1024, 4096], P('dp', 'expert')
The draws below stay inside these ranges and needn't reach their ends.
Inputs may be any that keep to these rules, and one draw needn't show every extreme that they name: `routing`: each row names two different experts. Within the 256 rows of one group, no expert is named by more than 192 rows, a bound that some block reaches.
All inputs are finite; a program needn't handle non-finite values.
Results may differ from the reference program's by a relative error of at most 0.02.
Values may be sent and summed in bfloat16 or wider, within the bound.
A program may use at most 64 MiB of HBM per device.

```python
import math
import jax
import jax.numpy as jnp
import numpy as np
from jax import lax

D = 4096
FF = 8192
GROUP = 256
EXPERTS = 4
CAP = 192
TOKENS = 1024
N_DP = 4
N_EXPERT = 8


def strengthened(result, rng, source, target, blocks, factor):
    owner, partner = [(jnp.arange(result.shape[position]) // (result.shape[position] // blocks)).reshape([-1 if axis == position else 1 for axis in range(result.ndim)]) for position in (source, target)]
    chosen = jax.random.permutation(rng, blocks)[partner]
    strong = (owner == chosen) | (owner == (partner + blocks // 2) % blocks)
    return jnp.where(strong, factor * result, result)


def shard_levels(rng, shape, pieces, low, high):
    def one(position, blocks):
        heights = jax.random.uniform(jax.random.fold_in(jax.random.fold_in(rng, 6), position), (blocks,), jnp.float32, low / len(pieces), high / len(pieces))
        return jnp.repeat(jnp.exp(heights), shape[position] // blocks).reshape((-1,) + (1,) * (len(shape) - position - 1))

    factor_of = one(*pieces[0])
    for cut in pieces[1:]:
        factor_of = factor_of * one(*cut)
    return factor_of


def assign_block(stream_key, own, number, rows, count, top, bound, slope):
    sequence = jax.random.permutation(stream_key, count)
    crowded, ordinary = portions_of(count, rows * top, bound, slope, True), portions_of(count, rows * top, bound, slope, False)
    places = jnp.arange(count)

    def named(sizes, turn):
        used = int((sizes > 0).sum())
        fixed = max(1, used // 4)
        passed = fixed + (places - fixed + turn * (used - fixed)) % max(1, count - fixed)
        return jnp.zeros((count,), jnp.int32).at[sequence[jnp.where(places < fixed, places, passed)]].set(jnp.asarray(sizes, jnp.int32))

    sizes = jnp.where(number % 4 == 0, named(crowded, number // 4), named(ordinary, number - number // 4 - 1))
    mixed = jax.random.permutation(jax.random.fold_in(own, 3), count)
    donor, sink = mixed[0:count // 2 * 2:2], mixed[1:count // 2 * 2:2]
    room = jnp.minimum(sizes[donor] - 1, bound - sizes[sink]) // 2
    room = jnp.where((donor == sequence[0]) | (sink == sequence[0]) | (sizes[sink] == 0), 0, jnp.maximum(room, 0))
    passed = jax.random.randint(jax.random.fold_in(own, 4), (count // 2,), 0, 1 << 20) % (room + 1)
    sizes = sizes.at[donor].add(-passed).at[sink].add(passed)
    items = jnp.searchsorted(jnp.cumsum(sizes), jnp.arange(rows * top), side="right").astype(jnp.int32)
    table = items.reshape(top, rows).T
    table = table[jax.random.permutation(jax.random.fold_in(own, 1), rows)]
    turn = jax.random.randint(jax.random.fold_in(own, 2), (rows, 1), 0, top)
    return jnp.take_along_axis(table, (jnp.arange(top)[None, :] + turn) % top, axis=1)


def portions_of(count, total, most, slope, full):
    weights = [(1 << 20) // math.isqrt(grade ** slope) + 1 for grade in range(1, count + 1)]
    largest = most if full else min(most, max(-(-total // count), total * weights[0] // sum(weights)))
    least = 1 if total - largest >= count - 1 else 0
    counts, surplus = [largest] + [least] * (count - 1), total - largest - least * (count - 1)
    while surplus > 0:
        candidates = [i for i in range(1, count) if counts[i] < largest] or [i for i in range(1, count) if counts[i] < most]
        whole, left = sum([weights[i] for i in candidates]), surplus
        for i in candidates:
            more = min(most - counts[i], max(1, left * weights[i] // whole), surplus)
            counts[i] = counts[i] + more
            surplus = surplus - more
    return np.array(counts)


def centred(rng, dims, deviation, most, shards=(), kind=jnp.bfloat16):
    result = deviation * jax.random.normal(rng, dims, jnp.float32)
    if shards:
        result = result * shard_levels(rng, dims, shards, -0.22, 0.18)
    return jnp.clip(result, -most, most).astype(kind)


def noise_with(key, shape, deviation, bound, shards, heavy, kind=jnp.bfloat16):
    array = deviation * jax.random.normal(key, shape, jnp.float32)
    if shards:
        array = array * shard_levels(key, shape, shards, -0.22, 0.18)
    return jnp.clip(strengthened(array, jax.random.fold_in(key, 3), *heavy), -bound, bound).astype(kind)


def setup_inputs(seed: int = 0) -> dict:
    streams_of = jax.random.split(jax.random.key(seed), 6)
    tokens = centred(streams_of[0], (TOKENS, D), 1.0, 6.0, ((0, 4), (1, 8)))
    routing_keys = jax.random.split(jax.random.fold_in(streams_of[1], 1), TOKENS // GROUP)
    routing_turns = jax.random.permutation(jax.random.fold_in(streams_of[1], 3), TOKENS // GROUP)
    routing = jax.vmap(lambda own, number: assign_block(jax.random.fold_in(streams_of[1], 2), own, number, GROUP, EXPERTS, 2, CAP, 2))(routing_keys, routing_turns).reshape((TOKENS, 2))
    gate_weight = centred(streams_of[2], (D, EXPERTS), D ** -0.5, 0.09375, ((0, 8),))
    expert_in = centred(streams_of[3], (EXPERTS, D, FF), D ** -0.5, 0.09375, ((0, 4), (2, 8)))
    expert_out = noise_with(streams_of[4], (EXPERTS, FF, D), (FF // 64) ** -0.5, 0.75, ((0, 4), (1, 8)), (1, 2, 8, 2.0))
    return {"tokens": tokens, "routing": routing, "gate_weight": gate_weight, "expert_in": expert_in, "expert_out": expert_out}


def slot_table(grouped):
    order = jnp.transpose(grouped, (0, 2, 1)).reshape(grouped.shape[0], -1)
    onehot = (order[:, :, None] == jnp.arange(EXPERTS, dtype=jnp.int32)[None, None, :]).astype(jnp.int32)
    before = jnp.cumsum(onehot, axis=1) - onehot
    slot_flat = jnp.sum(before * onehot, axis=-1).astype(jnp.int32)
    return jnp.transpose(slot_flat.reshape(grouped.shape[0], 2, -1), (0, 2, 1))


def reference(tokens, routing, gate_weight, expert_in, expert_out):
    logits = jnp.dot(tokens, gate_weight, preferred_element_type=jnp.float32)
    raised = jnp.exp(logits)
    softmax_all = raised / jnp.sum(raised, axis=-1, keepdims=True)
    chosen = jnp.take_along_axis(softmax_all, routing, axis=1).astype(jnp.bfloat16)
    grouped = routing.reshape(N_DP, GROUP, 2)
    slot_index = slot_table(grouped)
    group_ids = jnp.broadcast_to(jnp.arange(N_DP, dtype=jnp.int32)[:, None, None], (N_DP, GROUP, 2))
    token_rows = jnp.broadcast_to(tokens.reshape(N_DP, GROUP, 1, D), (N_DP, GROUP, 2, D))
    buffer = jnp.zeros((EXPERTS, N_DP, CAP, D), jnp.bfloat16)
    buffer = buffer.at[grouped, group_ids, slot_index].set(token_rows)
    width_block = FF // N_EXPERT

    def run_expert(packed):
        rows_in, weight_in, weight_out = packed
        flat_rows = rows_in.reshape(N_DP * CAP, D)
        hidden = jax.nn.gelu(jnp.dot(flat_rows, weight_in, preferred_element_type=jnp.float32), approximate=True).astype(jnp.bfloat16)

        def add_block(index, running):
            start = (index * width_block).astype(jnp.int32)
            left = lax.dynamic_slice_in_dim(hidden, start, width_block, 1)
            right = lax.dynamic_slice_in_dim(weight_out, start, width_block, 0)
            term = jnp.dot(left, right, preferred_element_type=jnp.float32).astype(jnp.bfloat16)
            term = lax.optimization_barrier(term)
            return running + term.astype(jnp.float32)

        summed = lax.fori_loop(0, N_EXPERT, add_block, jnp.zeros((N_DP * CAP, D), jnp.float32))
        return summed.astype(jnp.bfloat16).reshape(N_DP, CAP, D)

    expert_result = lax.map(run_expert, (buffer, expert_in, expert_out))
    picked = expert_result[grouped, group_ids, slot_index]
    weights = chosen.reshape(N_DP, GROUP, 2, 1).astype(jnp.float32)
    mixed = jnp.sum(picked.astype(jnp.float32) * weights, axis=2)
    return mixed.reshape(TOKENS, D).astype(jnp.bfloat16)
```

```python
import functools

import jax
import jax.numpy as jnp
from jax import lax
from jax.experimental import pallas as pl
from jax.experimental.pallas import tpu as pltpu
from jax.sharding import PartitionSpec as P


def softmax_rows(logits):
    raised = jnp.exp(logits)
    return raised / jnp.sum(raised, axis=-1, keepdims=True)


def pick_chosen(softmax_all, picks):
    experts = softmax_all.shape[1]
    labels = lax.broadcasted_iota(jnp.int32, (picks.shape[0], 2, experts), 2)
    selected = labels == picks[:, :, None]
    return jnp.sum(jnp.where(selected, softmax_all[:, None, :], 0.0), axis=-1).astype(jnp.bfloat16)


def expert_rows(block_rows, weight_in, weight_out):
    sources = block_rows.shape[0]
    slots_here = block_rows.shape[1]
    width_local = block_rows.shape[2]
    flat_rows = block_rows.reshape(sources * slots_here, width_local)
    pre_act = jnp.dot(
        lax.all_gather(flat_rows, "expert", axis=1, tiled=True),
        weight_in,
        preferred_element_type=jnp.float32,
    )
    hidden = jax.nn.gelu(pre_act, approximate=True).astype(jnp.bfloat16)
    partial_out = jnp.dot(hidden, weight_out, preferred_element_type=jnp.float32)
    summed = lax.psum_scatter(
        partial_out.astype(jnp.bfloat16), "expert", scatter_dimension=1, tiled=True
    )
    return summed.reshape(sources, slots_here, width_local)


def slots_plan(tokens, routing, gate_weight, expert_in, expert_out):
    group_size = tokens.shape[0]
    width_local = tokens.shape[1]
    experts = gate_weight.shape[1]
    dp_count = lax.axis_size("dp")
    capacity = 3 * group_size // dp_count
    weight_in = expert_in[0]
    weight_out = expert_out[0]
    partial_logits = jnp.dot(tokens, gate_weight, preferred_element_type=jnp.float32)
    logits = lax.psum(partial_logits, "expert")
    chosen = pick_chosen(softmax_rows(logits), routing)
    order = jnp.concatenate([routing[:, 0], routing[:, 1]], axis=0)
    labels = lax.broadcasted_iota(jnp.int32, (2 * group_size, experts), 1)
    onehot = (labels == order[:, None]).astype(jnp.int32)
    before = jnp.cumsum(onehot, axis=0) - onehot
    slot_flat = jnp.sum(before * onehot, axis=1)
    slot_index = jnp.stack([slot_flat[:group_size], slot_flat[group_size:]], axis=1)
    target = routing * capacity + slot_index
    columns = lax.broadcasted_iota(jnp.int32, (group_size, experts * capacity), 1)
    first_hit = columns == target[:, 0:1]
    second_hit = columns == target[:, 1:2]
    assign = jnp.logical_or(first_hit, second_hit).astype(jnp.bfloat16)
    outgoing = jnp.einsum("gs,gd->sd", assign, tokens, preferred_element_type=jnp.float32)
    outgoing = outgoing.astype(jnp.bfloat16).reshape(experts, capacity, width_local)
    incoming = lax.all_to_all(outgoing, "dp", split_axis=0, concat_axis=0, tiled=True)
    processed = expert_rows(incoming, weight_in, weight_out)
    returned_rows = lax.all_to_all(processed, "dp", split_axis=0, concat_axis=0, tiled=True)
    zero_weight = jnp.zeros((), jnp.bfloat16)
    combine = jnp.where(first_hit, chosen[:, 0:1], zero_weight) + jnp.where(
        second_hit, chosen[:, 1:2], zero_weight
    )
    mixed = jnp.dot(
        combine,
        returned_rows.reshape(experts * capacity, width_local),
        preferred_element_type=jnp.float32,
    )
    return mixed.astype(jnp.bfloat16)


MESH = pl.DeviceIdType.MESH
F32 = jnp.float32
BF16 = jnp.bfloat16


def whole_kernel(
    experts,
    tok, gate_in, routes, win_hbm, wout_hbm, out,
    extra,
    xs, gates, picks_of, win, wout, pre, logit, hidden, give, take, part,
    from_side, from_corner, from_pair, line_pair, line_mid,
    wsem, xy_s, xy_r, relay_s, relay_r, zp_s, zm_s, z_r, pass_s, pass_r, ds, dr,
    es, er, ep_s, em_s, ez_r, eds, edr,
    ps, pr, side_s, side_r, corner_s, corner_r, pair_s, pair_r, lp_s, lp_r, lm_s, lm_r,
):
    dp, me = lax.axis_index("dp"), lax.axis_index("expert")
    z, k = me // 2, me % 2
    depth = lax.axis_size("expert") // 2
    group, width = tok.shape
    half = group // 2
    gx, gy = dp // 2 * 2 + 1 - dp % 2, (1 - dp // 2) * 2 + dp % 2
    gd = 3 - dp
    upper = z // 2
    near = z * (1 - upper) + (depth - 1 - z) * upper
    mid, edge = near == 1, near == 0
    rows = (pl.ds(0, half), pl.ds(half, half))
    partner = (dp, z * 2 + 1 - k)

    def at(q):
        return q * (1 - upper) + (depth - 1 - q) * upper

    def slot(i):
        return at(lax.rem(near + i, depth))

    def turned(j):
        return at(j + 2 * near)

    def passed(j):
        return at(j + 2 * (1 - near))

    pair, across = (dp, at(1 - near) * 2 + k), (dp, (depth - 1 - z) * 2 + k)
    side = ((gx, me), (gy, me))
    waits = []

    def make(src, dst, s_sem, r_sem, who):
        return pltpu.make_async_remote_copy(src, dst, s_sem, r_sem, device_id=who, device_id_type=MESH)

    def send(src, dst, s_sem, r_sem, who):
        copy = make(src, dst, s_sem, r_sem, who)
        copy.start()
        waits.append((None, copy))

    def send_if(role, src, dst, s_sem, r_sem, who):
        copy = make(src, dst, s_sem, r_sem, who)
        pl.when(role)(copy.start)
        waits.append((role, copy))

    def got(ref, s_sem, r_sem):
        make(ref, ref, s_sem, r_sem, partner).wait_recv()

    load_in = pltpu.make_async_copy(win_hbm.at[0], win, wsem.at[0])
    load_out = pltpu.make_async_copy(wout_hbm.at[0], wout, wsem.at[1])
    barrier = pltpu.get_barrier_semaphore()
    for who in (partner, *side, (gd, me), pair):
        pl.semaphore_signal(barrier, inc=1, device_id=who, device_id_type=MESH)

    @pl.when(mid)
    def _():
        pl.semaphore_signal(barrier, inc=1, device_id=across, device_id_type=MESH)

    load_in.start()
    load_out.start()
    pl.semaphore_wait(barrier, 5 + near)

    def mine(i):
        return tok if i == 0 else xs.at[dp, slot(i), k]

    def direct(i, h, role=None):
        for d in range(2):
            args = (mine(i).at[rows[h]], xs.at[dp, slot(i), k, rows[h]], xy_s.at[i, d, h], xy_r.at[i, d, h], side[d])
            if role is None:
                send(*args)
            else:
                pl.when(role)(make(*args).start)

    def direct_last(h, role):
        direct(3, h, role)

    def to_pair(i, h, n, s):
        zz = slot(i)
        return make(mine(i).at[rows[h]], xs.at[dp, zz, k, rows[h]], zp_s.at[n, h], z_r.at[s, h], pair)

    def to_mid(i, h, n):
        zz = slot(i)
        return make(mine(i).at[rows[h]], xs.at[dp, zz, k, rows[h]], zm_s.at[n, h], z_r.at[n, h], across)

    def line_in(i, h):
        got(xs.at[dp, slot(i), k, rows[h]], zp_s.at[0, h], z_r.at[i - 1, h])

    def cross(i, t, g, zz):
        block = tok if i == 0 and t == 0 else xs.at[g, zz, k]
        send(block, xs.at[g, zz, k], ds.at[i, t], dr.at[i, t], partner)

    def crossed(i, t, g, zz):
        got(xs.at[g, zz, 1 - k], ds.at[i, t], dr.at[i, t])

    def sides_in(i, h):
        for d, g in enumerate((gx, gy)):
            got(xs.at[g, slot(i), k, rows[h]], xy_s.at[i, d, h], xy_r.at[i, d, h])

    def relay(j, role=None):
        zz = turned(j)
        for n, (g, who) in enumerate(((gx, side[1]), (gy, side[0]))):
            block = xs.at[g, zz, k, rows[n]]
            args = (block, block, relay_s.at[j, n], relay_r.at[j, n], who)
            if role is None:
                send(*args)
            else:
                pl.when(role)(make(*args).start)

    def corner_in(j):
        zz = turned(j)
        for h in range(2):
            block = xs.at[gd, zz, k, rows[h]]
            got(block, relay_s.at[j, h], relay_r.at[j, h])
            send(block, block, pass_s.at[j, h], pass_r.at[j, h], pair)
        cross(j, 3, gd, zz)

    def passed_in(j, h):
        got(xs.at[gd, passed(j), k, rows[h]], pass_s.at[j, h], pass_r.at[j, h])

    own_line = 2 - 2 * near
    for h in range(2):
        first = to_pair(0, h, 0, own_line)
        first.start()
        waits.append((None, first))
        second = to_mid(0, h, 0)
        pl.when(mid)(second.start)
        waits.append((mid, second))
        direct(0, h)
    cross(0, 0, dp, z)

    wide = lax.broadcasted_iota(jnp.int32, (8, experts), 0) == lax.broadcasted_iota(jnp.int32, (8, experts), 1)
    both = lax.broadcasted_iota(jnp.int32, (8, 2), 0) == lax.broadcasted_iota(jnp.int32, (8, 2), 1) + experts
    gate_rows = jnp.dot(jnp.where(wide, 1.0, 0.0).astype(BF16), gate_in[...], preferred_element_type=F32)
    route_rows = jnp.dot(
        jnp.where(both, 1.0, 0.0).astype(BF16), routes[...].astype(F32).astype(BF16), preferred_element_type=F32
    )
    extra[...] = gate_rows.astype(BF16)
    extra[:, :group] = (gate_rows[:, :group] + route_rows).astype(BF16)
    for i, who in enumerate((*side, (gd, me))):
        send(extra, picks_of.at[dp], es.at[i], er.at[i], who)
    send(extra, gates.at[z, k], ep_s.at[0], ez_r.at[own_line], pair)
    send_if(mid, extra, gates.at[z, k], em_s.at[0], ez_r.at[0], across)
    send(extra, gates.at[z, k], eds.at[0], edr.at[0], partner)
    picks_of[dp] = extra[...]
    gates[z, k] = extra[...]
    xs[dp, z, k] = tok[...]
    pre[...] = jnp.zeros_like(pre)
    logit[...] = jnp.zeros_like(logit)

    def gate_in_line(i):
        zz = slot(i)
        got(gates.at[zz, k], ep_s.at[0], ez_r.at[i - 1])
        send(gates.at[zz, k], gates.at[zz, k], eds.at[i], edr.at[i], partner)

    def gate_ready(i):
        got(gates.at[slot(i), 1 - k], eds.at[i], edr.at[i])

    def accumulate(g, zz):
        total, score = pre[g], logit[g]
        for kk in range(2):
            strip = pl.ds(pl.multiple_of((zz * 2 + kk) * width, width), width)
            block = xs[g, zz, kk]
            total += jnp.dot(block, win[strip, :], preferred_element_type=F32)
            score += lax.dot_general(gates[zz, kk], block, (((1,), (1,)), ((), ())), preferred_element_type=F32)
        pre[g] = total
        logit[g] = score

    def choose(c, options):
        chosen = options[-1]
        for n in range(len(options) - 2, -1, -1):
            chosen = jnp.where(c == n, options[n], chosen)
        return chosen

    def several(count, fn):
        lax.fori_loop(0, count, lambda c, carry: fn(c) or carry, 0)

    def absorb(*which):
        for i, t, g, zz in which:
            crossed(i, t, g, zz)
        gs, zs = [w[2] for w in which], [w[3] for w in which]
        several(len(which), lambda c: accumulate(choose(c, gs), choose(c, zs)))

    def from_own(i):
        return (i, 0, dp, slot(i))

    def from_x(i):
        return (i, 1, gx, slot(i))

    def from_y(i):
        return (i, 2, gy, slot(i))

    def from_turned(j):
        return (j, 3, gd, turned(j))

    def from_passed(j):
        return (2 + j, 3, gd, passed(j))

    def forward(i, h, n, s):
        copy = to_pair(i, h, n, s)
        pl.when(mid)(copy.start)
        waits.append((mid, copy))

    def outward(h):
        copy = to_mid(3, h, 1)

        @pl.when(mid)
        def _():
            line_in(3, h)
            copy.start()

        waits.append((mid, copy))

    def cross_sides(i):
        cross(i, 1, gx, slot(i))
        cross(i, 2, gy, slot(i))

    for h in range(2):
        line_in(1, h)
        forward(1, h, 1, 1)
        direct(1, h)
        outward(h)
        sides_in(0, h)
    cross_sides(0)
    cross(1, 0, dp, slot(1))
    gate_in_line(1)
    send_if(mid, gates.at[slot(1), k], gates.at[slot(1), k], ep_s.at[1], ez_r.at[1], pair)
    gate_line_3 = make(gates.at[slot(3), k], gates.at[slot(3), k], em_s.at[1], ez_r.at[1], across)

    @pl.when(mid)
    def _():
        got(gates.at[slot(3), k], ep_s.at[0], ez_r.at[2])
        gate_line_3.start()

    waits.append((mid, gate_line_3))
    for i, g in enumerate((gx, gy, gd)):
        got(picks_of.at[g], es.at[i], er.at[i])
    load_in.wait()
    gate_ready(0)
    absorb(from_own(0))
    line_in(2, 0)
    forward(2, 0, 2, 2)
    direct(2, 0)
    sides_in(1, 0)
    absorb(from_x(0))
    line_in(2, 1)
    forward(2, 1, 2, 2)
    gate_in_line(2)
    send_if(mid, gates.at[slot(2), k], gates.at[slot(2), k], ep_s.at[2], ez_r.at[2], pair)
    sides_in(1, 1)
    relay(0)
    direct(2, 1)
    relay(1, edge)
    cross_sides(1)
    cross(2, 0, dp, slot(2))
    gate_ready(1)
    absorb(from_y(0), from_own(1))
    sides_in(2, 0)

    @pl.when(edge)
    def _():
        line_in(3, 0)
        direct_last(0, True)

    absorb(from_x(1))

    @pl.when(edge)
    def _():
        got(gates.at[slot(3), k], ep_s.at[0], ez_r.at[2])

    send(gates.at[slot(3), k], gates.at[slot(3), k], eds.at[3], edr.at[3], partner)
    corner_in(0)

    @pl.when(edge)
    def _():
        line_in(3, 1)
        direct_last(1, True)

    gate_ready(2)
    absorb(from_y(1))
    sides_in(2, 1)
    relay(1, mid)
    direct(3, 0, mid)
    direct(3, 1, mid)
    cross_sides(2)
    cross(3, 0, dp, slot(3))
    absorb(from_turned(0), from_own(2))
    passed_in(0, 0)
    corner_in(1)
    passed_in(0, 1)
    cross(2, 3, gd, passed(0))
    gate_ready(3)
    absorb(from_x(2), from_y(2))
    sides_in(3, 0)
    passed_in(1, 0)
    absorb(from_turned(1), from_passed(0), from_own(3))
    sides_in(3, 1)
    cross_sides(3)
    passed_in(1, 1)
    cross(3, 3, gd, passed(1))
    for h in range(2):
        for d in range(2):
            waits.append((None, make(mine(3).at[rows[h]], mine(3).at[rows[h]], xy_s.at[3, d, h], xy_r.at[3, d, h], side[d])))
        waits.append((None, make(mine(3).at[rows[h]], mine(3).at[rows[h]], relay_s.at[1, h], relay_r.at[1, h], side[0])))

    def activate(g):
        score = logit[g]
        row = lax.broadcasted_iota(jnp.int32, score.shape, 0)
        raised = jnp.where(row < experts, jnp.exp(score), 0.0)
        chance = raised / jnp.sum(raised, axis=0, keepdims=True)
        own = jnp.sum(jnp.where(row == dp, chance, 0.0), axis=0, keepdims=True)
        picks = picks_of[g][:, :group].astype(F32)
        named = jnp.logical_and(jnp.logical_or(row == experts, row == experts + 1), picks == dp.astype(F32))
        hit = jnp.sum(jnp.where(named, 1.0, 0.0), axis=0, keepdims=True)
        scale = own.astype(BF16).astype(F32) * hit
        column = jnp.transpose(jnp.broadcast_to(scale, (128, group)))[:, :1]
        acted = jax.nn.gelu(pre[g], approximate=True)
        hidden[g] = (acted * column).astype(BF16)

    def product(g, zz, kk):
        cols = pl.ds(pl.multiple_of((zz * 2 + kk) * width, width), width)
        return jnp.dot(hidden[g], wout[:, cols], preferred_element_type=F32)

    order = [
        (gx, slot(3)), (gy, slot(3)), (gd, passed(1)),
        (gx, slot(2)), (gy, slot(2)), (gd, passed(0)), (gd, turned(1)),
        (dp, slot(3)), (gd, turned(0)),
        (gx, slot(1)), (gy, slot(1)), (dp, slot(2)),
        (dp, slot(1)), (gx, slot(0)), (gy, slot(0)), (dp, slot(0)),
    ]

    def lend(n, g, zz):
        give[zz, g] = product(g, zz, 1 - k).astype(BF16)
        make(give.at[zz, g], take.at[zz, g], ps.at[n], pr.at[n], partner).start()

    def keep(g, zz):
        part[zz, g] = (product(g, zz, k) + take[zz, g].astype(F32)).astype(BF16)

    def lend_all(lo, hi):
        gs, zs = [w[0] for w in order[lo:hi]], [w[1] for w in order[lo:hi]]
        several(hi - lo, lambda c: lend(lo + c, choose(c, gs), choose(c, zs)))

    def taken(n):
        g, zz = order[n]
        got(take.at[zz, g], ps.at[n], pr.at[n])

    def keep_all(lo, hi):
        for n in range(lo, hi):
            taken(n)
        gs, zs = [w[0] for w in order[lo:hi]], [w[1] for w in order[lo:hi]]
        several(hi - lo, lambda c: keep(choose(c, gs), choose(c, zs)))

    for n in range(len(order)):
        g, zz = order[n]
        waits.append((None, make(give.at[zz, g], take.at[zz, g], ps.at[n], pr.at[n], partner)))

    def to_side(i, d, h):
        g = (gx, gy)[d]
        send(part.at[slot(i), g, rows[h]], from_side.at[i, d, h], side_s.at[i, d, h], side_r.at[i, d, h], side[d])

    def to_corner(j, h):
        zz = turned(j)
        got(from_pair.at[j, h], pair_s.at[j, h], pair_r.at[j, h])
        part[zz, gd, rows[h]] = (part[zz, gd, rows[h]].astype(F32) + from_pair[j, h].astype(F32)).astype(BF16)
        send(part.at[zz, gd, rows[h]], from_corner.at[j, h], corner_s.at[j, h], corner_r.at[j, h], side[h])

    def corner_add(j):
        zz = turned(j)
        for h, g in ((0, gy), (1, gx)):
            got(from_corner.at[j, h], corner_s.at[j, h], corner_r.at[j, h])
            part[zz, g, rows[h]] = (part[zz, g, rows[h]].astype(F32) + from_corner[j, h].astype(F32)).astype(BF16)

    def send_passed(j):
        zz = passed(j)
        for h in range(2):
            send(part.at[zz, gd, rows[h]], from_pair.at[j, h], pair_s.at[j, h], pair_r.at[j, h], pair)

    def gathered(i, h):
        total = part[slot(i), dp, rows[h]].astype(F32)
        for d in range(2):
            got(from_side.at[i, d, h], side_s.at[i, d, h], side_r.at[i, d, h])
            total += from_side[i, d, h].astype(F32)
        return total

    def line_pair_in(n, h):
        got(line_pair.at[n, h], lp_s.at[0, h], lp_r.at[n, h])
        return line_pair[n, h].astype(F32)

    def line_mid_in(n, h):
        got(line_mid.at[n, h], lm_s.at[0, h], lm_r.at[n, h])
        return line_mid[n, h].astype(F32)

    def line_to_pair(i, h, n):
        return make(part.at[slot(i), dp, rows[h]], line_pair.at[n, h], lp_s.at[n, h], lp_r.at[n, h], pair)

    def line_to_mid(i, h, n):
        return make(part.at[slot(i), dp, rows[h]], line_mid.at[n, h], lm_s.at[n, h], lm_r.at[n, h], across)

    def settle(i):
        for h in range(2):
            total = gathered(i, h)
            zz = slot(i)
            to_pair_copy = line_to_pair(i, h, i - 1)

            @pl.when(edge)
            def _():
                part[zz, dp, rows[h]] = total.astype(BF16)
                to_pair_copy.start()

            waits.append((edge, to_pair_copy))
            if i == 3:

                @pl.when(mid)
                def _():
                    part[zz, dp, rows[h]] = total.astype(BF16)
            else:
                copy = line_to_mid(i, h, 2 - i)

                @pl.when(mid)
                def _():
                    part[zz, dp, rows[h]] = (total + line_pair_in(i, h)).astype(BF16)
                    copy.start()

                waits.append((mid, copy))

    def outer():
        for h in range(2):
            copy = line_to_pair(3, h, 0)

            @pl.when(mid)
            def _():
                zz = slot(3)
                came = line_mid_in(0, h)
                part[zz, dp, rows[h]] = (part[zz, dp, rows[h]].astype(F32) + came).astype(BF16)
                copy.start()

            waits.append((mid, copy))

    load_out.wait()
    for n, which in enumerate((from_x(3), from_y(3), from_passed(1))):
        absorb(which)
        activate(which[2])
        lend(n, *order[n])
    keep_all(0, 1)
    for h in range(2):
        to_side(3, 0, h)
    keep_all(1, 2)
    for h in range(2):
        to_side(3, 1, h)
    keep_all(2, 3)
    send_passed(1)
    activate(dp)
    lend_all(3, 7)
    keep_all(3, 7)
    to_side(2, 0, 0)
    to_side(2, 1, 1)
    send_passed(0)
    for h in range(2):
        to_corner(1, h)
    lend_all(7, 9)
    keep_all(7, 9)
    settle(3)
    for h in range(2):
        to_corner(0, h)
    lend_all(9, 12)
    pl.when(mid)(functools.partial(corner_add, 1))
    to_side(2, 0, 1)
    to_side(2, 1, 0)
    keep_all(9, 12)
    pl.when(edge)(functools.partial(corner_add, 1))
    to_side(1, 0, 0)
    to_side(1, 1, 1)
    lend_all(12, 16)
    pl.when(mid)(functools.partial(corner_add, 0))
    to_side(1, 0, 1)
    to_side(1, 1, 0)
    settle(2)
    keep_all(12, 16)
    pl.when(edge)(functools.partial(corner_add, 0))
    for h in range(2):
        to_side(0, 0, h)
        to_side(0, 1, h)
    settle(1)
    outer()
    for h in range(2):
        total = gathered(0, h)

        @pl.when(mid)
        def _():
            out[rows[h]] = (total + line_pair_in(0, h) + line_mid_in(1, h)).astype(BF16)

        @pl.when(edge)
        def _():
            out[rows[h]] = (total + line_pair_in(0, h)).astype(BF16)

    for role, copy in waits:
        if role is None:
            copy.wait_send()
        else:
            pl.when(role)(copy.wait_send)


def tokens_plan(tokens, routing, gate_weight, expert_in, expert_out):
    group, width = tokens.shape
    depth = lax.axis_size("expert") // 2
    experts = gate_weight.shape[1]
    model, inner = expert_in.shape[1:]
    half = group // 2
    vmem = pltpu.VMEM
    dma = pltpu.SemaphoreType.DMA
    return pl.pallas_call(
        functools.partial(whole_kernel, experts),
        out_shape=jax.ShapeDtypeStruct((group, width), BF16),
        in_specs=[pl.BlockSpec(memory_space=vmem)] * 3 + [pl.BlockSpec(memory_space=pl.ANY)] * 2,
        out_specs=pl.BlockSpec(memory_space=vmem),
        scratch_shapes=[
            vmem((8, width), BF16),
            vmem((4, depth, 2, group, width), BF16),
            vmem((depth, 2, 8, width), BF16),
            vmem((4, 8, width), BF16),
            vmem((model, inner), BF16),
            vmem((inner, model), BF16),
            vmem((4, group, inner), F32),
            vmem((4, 8, group), F32),
            vmem((4, group, inner), BF16),
            vmem((depth, 4, group, width), BF16),
            vmem((depth, 4, group, width), BF16),
            vmem((depth, 4, group, width), BF16),
            vmem((depth, 2, 2, half, width), BF16),
            vmem((2, 2, half, width), BF16),
            vmem((2, 2, half, width), BF16),
            vmem((3, 2, half, width), BF16),
            vmem((2, 2, half, width), BF16),
            dma((2,)),
            dma((depth, 2, 2)), dma((depth, 2, 2)),
            dma((2, 2)), dma((2, 2)),
            dma((3, 2)), dma((2, 2)), dma((3, 2)),
            dma((2, 2)), dma((2, 2)),
            dma((depth, 4)), dma((depth, 4)),
            dma((3,)), dma((3,)),
            dma((3,)), dma((2,)), dma((3,)),
            dma((depth,)), dma((depth,)),
            dma((4 * depth,)), dma((4 * depth,)),
            dma((depth, 2, 2)), dma((depth, 2, 2)),
            dma((2, 2)), dma((2, 2)),
            dma((2, 2)), dma((2, 2)),
            dma((3, 2)), dma((3, 2)),
            dma((2, 2)), dma((2, 2)),
        ],
        compiler_params=pltpu.CompilerParams(
            collective_id=0, has_side_effects=True, vmem_limit_bytes=63 * 1024 * 1024
        ),
    )(tokens, gate_weight.T, routing.T, expert_in, expert_out)


def solution(mesh):
    placed = (
        P("dp", "expert"),
        P("dp", None),
        P("expert", None),
        P("dp", None, "expert"),
        P("dp", "expert", None),
    )
    body = tokens_plan if tuple(mesh.shape.values()) == (4, 8) else slots_plan
    return jax.shard_map(
        body, mesh=mesh, in_specs=placed, out_specs=P("dp", "expert"), check_vma=False
    )
```

```python
import functools

import jax
import jax.numpy as jnp
from jax import lax
from jax.experimental import pallas as pl
from jax.experimental.pallas import tpu as pltpu
from jax.sharding import PartitionSpec as P


def softmax_rows(logits):
    raised = jnp.exp(logits)
    return raised / jnp.sum(raised, axis=-1, keepdims=True)


def pick_chosen(softmax_all, picks):
    experts = softmax_all.shape[1]
    labels = lax.broadcasted_iota(jnp.int32, (picks.shape[0], 2, experts), 2)
    selected = labels == picks[:, :, None]
    return jnp.sum(jnp.where(selected, softmax_all[:, None, :], 0.0), axis=-1).astype(jnp.bfloat16)


def expert_rows(block_rows, weight_in, weight_out):
    sources = block_rows.shape[0]
    slots_here = block_rows.shape[1]
    width_local = block_rows.shape[2]
    flat_rows = block_rows.reshape(sources * slots_here, width_local)
    pre_act = jnp.dot(
        lax.all_gather(flat_rows, "expert", axis=1, tiled=True),
        weight_in,
        preferred_element_type=jnp.float32,
    )
    hidden = jax.nn.gelu(pre_act, approximate=True).astype(jnp.bfloat16)
    partial_out = jnp.dot(hidden, weight_out, preferred_element_type=jnp.float32)
    summed = lax.psum_scatter(
        partial_out.astype(jnp.bfloat16), "expert", scatter_dimension=1, tiled=True
    )
    return summed.reshape(sources, slots_here, width_local)


def slots_plan(tokens, routing, gate_weight, expert_in, expert_out):
    group_size = tokens.shape[0]
    width_local = tokens.shape[1]
    experts = gate_weight.shape[1]
    dp_count = lax.axis_size("dp")
    capacity = 3 * group_size // dp_count
    weight_in = expert_in[0]
    weight_out = expert_out[0]
    partial_logits = jnp.dot(tokens, gate_weight, preferred_element_type=jnp.float32)
    logits = lax.psum(partial_logits, "expert")
    chosen = pick_chosen(softmax_rows(logits), routing)
    order = jnp.concatenate([routing[:, 0], routing[:, 1]], axis=0)
    labels = lax.broadcasted_iota(jnp.int32, (2 * group_size, experts), 1)
    onehot = (labels == order[:, None]).astype(jnp.int32)
    before = jnp.cumsum(onehot, axis=0) - onehot
    slot_flat = jnp.sum(before * onehot, axis=1)
    slot_index = jnp.stack([slot_flat[:group_size], slot_flat[group_size:]], axis=1)
    target = routing * capacity + slot_index
    columns = lax.broadcasted_iota(jnp.int32, (group_size, experts * capacity), 1)
    first_hit = columns == target[:, 0:1]
    second_hit = columns == target[:, 1:2]
    assign = jnp.logical_or(first_hit, second_hit).astype(jnp.bfloat16)
    outgoing = jnp.einsum("gs,gd->sd", assign, tokens, preferred_element_type=jnp.float32)
    outgoing = outgoing.astype(jnp.bfloat16).reshape(experts, capacity, width_local)
    incoming = lax.all_to_all(outgoing, "dp", split_axis=0, concat_axis=0, tiled=True)
    processed = expert_rows(incoming, weight_in, weight_out)
    returned_rows = lax.all_to_all(processed, "dp", split_axis=0, concat_axis=0, tiled=True)
    zero_weight = jnp.zeros((), jnp.bfloat16)
    combine = jnp.where(first_hit, chosen[:, 0:1], zero_weight) + jnp.where(
        second_hit, chosen[:, 1:2], zero_weight
    )
    mixed = jnp.dot(
        combine,
        returned_rows.reshape(experts * capacity, width_local),
        preferred_element_type=jnp.float32,
    )
    return mixed.astype(jnp.bfloat16)


MESH = pl.DeviceIdType.MESH
F32 = jnp.float32
BF16 = jnp.bfloat16


def whole_kernel(
    experts,
    tok_hbm, gate_hbm, routes_hbm, win_hbm, wout_hbm, out,
    extra, gate_in, routes,
    xs, gates, picks_of, win, wout, pre, logit, hidden, give, take, part,
    from_side, from_corner, from_pair, line_pair, line_mid,
    wsem, xy_s, xy_r, relay_s, relay_r, zp_s, zm_s, z_r, pass_s, pass_r, ds, dr,
    es, er, ep_s, em_s, ez_r, eds, edr,
    ps, pr, hs, hr, ths, thr, side_s, side_r, corner_s, corner_r, pair_s, pair_r, lp_s, lp_r, lm_s, lm_r,
):
    dp, me = lax.axis_index("dp"), lax.axis_index("expert")
    z, k = me // 2, me % 2
    depth = lax.axis_size("expert") // 2
    group, width = tok_hbm.shape
    half = group // 2
    gx, gy = dp // 2 * 2 + 1 - dp % 2, (1 - dp // 2) * 2 + dp % 2
    gd = 3 - dp
    upper = z // 2
    near = z * (1 - upper) + (depth - 1 - z) * upper
    mid, edge = near == 1, near == 0
    rows = (pl.ds(0, half), pl.ds(half, half))
    partner = (dp, z * 2 + 1 - k)

    def at(q):
        return q * (1 - upper) + (depth - 1 - q) * upper

    def slot(i):
        return at(lax.rem(near + i, depth))

    def turned(j):
        return at(j + 2 * near)

    def passed(j):
        return at(j + 2 * (1 - near))

    pair, across = (dp, at(1 - near) * 2 + k), (dp, (depth - 1 - z) * 2 + k)
    side = ((gx, me), (gy, me))
    waits = []

    def make(src, dst, s_sem, r_sem, who):
        return pltpu.make_async_remote_copy(src, dst, s_sem, r_sem, device_id=who, device_id_type=MESH)

    def send(src, dst, s_sem, r_sem, who):
        copy = make(src, dst, s_sem, r_sem, who)
        copy.start()
        waits.append((None, copy))

    def send_if(role, src, dst, s_sem, r_sem, who):
        copy = make(src, dst, s_sem, r_sem, who)
        pl.when(role)(copy.start)
        waits.append((role, copy))

    def got(ref, s_sem, r_sem):
        make(ref, ref, s_sem, r_sem, partner).wait_recv()

    own = xs.at[dp, z, k]
    small = [
        pltpu.make_async_copy(src, dst, wsem.at[2 + i])
        for i, (src, dst) in enumerate(((tok_hbm, own), (gate_hbm, gate_in), (routes_hbm, routes)))
    ]
    load_in = pltpu.make_async_copy(win_hbm.at[0], win, wsem.at[0])
    load_out = pltpu.make_async_copy(wout_hbm.at[0], wout, wsem.at[1])
    barrier = pltpu.get_barrier_semaphore()
    for who in (partner, *side, (gd, me), pair):
        pl.semaphore_signal(barrier, inc=1, device_id=who, device_id_type=MESH)

    @pl.when(mid)
    def _():
        pl.semaphore_signal(barrier, inc=1, device_id=across, device_id_type=MESH)

    for copy in (*small, load_in, load_out):
        copy.start()
    pl.semaphore_wait(barrier, 5 + near)
    small[0].wait()

    def mine(i):
        return own if i == 0 else xs.at[dp, slot(i), k]

    def span(h):
        return pl.ds(pl.multiple_of(h * half, half), half)

    def turn(i, d, h):
        return h + near * (1 - 2 * h) if i == 2 and d == 1 else h

    def direct(i, h, role=None, ways=(0, 1)):
        for d in ways:
            hh = turn(i, d, h)
            copy = make(
                mine(i).at[span(hh)], xs.at[dp, slot(i), k, span(hh)], xy_s.at[i, d, hh], xy_r.at[i, d, hh], side[d]
            )
            if role is None:
                copy.start()
            else:
                pl.when(role)(copy.start)

    def to_pair(i, h, n, s):
        zz = slot(i)
        return make(mine(i).at[rows[h]], xs.at[dp, zz, k, rows[h]], zp_s.at[n, h], z_r.at[s, h], pair)

    def to_mid(i, h, n):
        zz = slot(i)
        return make(mine(i).at[rows[h]], xs.at[dp, zz, k, rows[h]], zm_s.at[n, h], z_r.at[n, h], across)

    def line_in(i, h):
        got(xs.at[dp, slot(i), k, rows[h]], zp_s.at[0, h], z_r.at[i - 1, h])

    def cross(i, t, g, zz):
        block = xs.at[g, zz, k]
        send(block, xs.at[g, zz, k], ds.at[i, t], dr.at[i, t], partner)

    def crossed(i, t, g, zz):
        got(xs.at[g, zz, 1 - k], ds.at[i, t], dr.at[i, t])

    def cross_half(n, h, g, zz):
        block = xs.at[g, zz, k, rows[h]]
        send(block, block, hs.at[n, h], hr.at[n, h], partner)

    def sides_in(i, h):
        for d, g in enumerate((gx, gy)):
            hh = turn(i, d, h)
            got(xs.at[g, slot(i), k, span(hh)], xy_s.at[i, d, hh], xy_r.at[i, d, hh])

    def relay(j, role=None, ways=(0, 1)):
        zz = turned(j)
        for n in ways:
            g, who = ((gx, side[1]), (gy, side[0]))[n]
            block = xs.at[g, zz, k, rows[n]]
            copy = make(block, block, relay_s.at[j, n], relay_r.at[j, n], who)
            if role is None:
                copy.start()
            else:
                pl.when(role)(copy.start)

    def corner_in(j):
        zz = turned(j)
        for h in range(2):
            block = xs.at[gd, zz, k, rows[h]]
            got(block, relay_s.at[j, h], relay_r.at[j, h])
            send(block, block, pass_s.at[j, h], pass_r.at[j, h], pair)
        cross(j, 3, gd, zz)

    def passed_in(j, h):
        got(xs.at[gd, passed(j), k, rows[h]], pass_s.at[j, h], pass_r.at[j, h])

    own_line = 2 - 2 * near
    for h in range(2):
        first = to_pair(0, h, 0, own_line)
        first.start()
        waits.append((None, first))
        second = to_mid(0, h, 0)
        pl.when(mid)(second.start)
        waits.append((mid, second))
        direct(0, h)
    cross(0, 0, dp, z)

    small[1].wait()
    small[2].wait()
    wide = lax.broadcasted_iota(jnp.int32, (8, experts), 0) == lax.broadcasted_iota(jnp.int32, (8, experts), 1)
    both = lax.broadcasted_iota(jnp.int32, (8, 2), 0) == lax.broadcasted_iota(jnp.int32, (8, 2), 1) + experts
    gate_rows = jnp.dot(jnp.where(wide, 1.0, 0.0).astype(BF16), gate_in[...], preferred_element_type=F32)
    route_rows = jnp.dot(
        jnp.where(both, 1.0, 0.0).astype(BF16), routes[...].astype(F32).astype(BF16), preferred_element_type=F32
    )
    extra[...] = gate_rows.astype(BF16)
    extra[:, :group] = (gate_rows[:, :group] + route_rows).astype(BF16)
    for i, who in enumerate((*side, (gd, me))):
        send(extra, picks_of.at[dp], es.at[i], er.at[i], who)
    send(extra, gates.at[z, k], ep_s.at[0], ez_r.at[own_line], pair)
    send_if(mid, extra, gates.at[z, k], em_s.at[0], ez_r.at[0], across)
    send(extra, gates.at[z, k], eds.at[0], edr.at[0], partner)
    picks_of[dp] = extra[...]
    gates[z, k] = extra[...]
    pre[...] = jnp.zeros_like(pre)
    logit[...] = jnp.zeros_like(logit)

    def gate_in_line(i):
        zz = slot(i)
        got(gates.at[zz, k], ep_s.at[0], ez_r.at[i - 1])
        send(gates.at[zz, k], gates.at[zz, k], eds.at[i], edr.at[i], partner)

    def gate_ready(i):
        got(gates.at[slot(i), 1 - k], eds.at[i], edr.at[i])

    def accumulate(g, zz):
        total, score = pre[g], logit[g]
        for kk in range(2):
            strip = pl.ds(pl.multiple_of((zz * 2 + kk) * width, width), width)
            block = xs[g, zz, kk]
            total += jnp.dot(block, win[strip, :], preferred_element_type=F32)
            score += lax.dot_general(gates[zz, kk], block, (((1,), (1,)), ((), ())), preferred_element_type=F32)
        pre[g] = total
        logit[g] = score

    def choose(c, options):
        chosen = options[-1]
        for n in range(len(options) - 2, -1, -1):
            chosen = jnp.where(c == n, options[n], chosen)
        return chosen

    def several(count, fn):
        lax.fori_loop(0, count, lambda c, carry: fn(c) or carry, 0)

    def absorb(*which):
        for i, t, g, zz in which:
            crossed(i, t, g, zz)
        gs, zs = [w[2] for w in which], [w[3] for w in which]
        several(len(which), lambda c: accumulate(choose(c, gs), choose(c, zs)))

    def from_own(i):
        return (i, 0, dp, slot(i))

    def from_x(i):
        return (i, 1, gx, slot(i))

    def from_y(i):
        return (i, 2, gy, slot(i))

    def from_turned(j):
        return (j, 3, gd, turned(j))

    def from_passed(j):
        return (2 + j, 3, gd, passed(j))

    def forward(i, h, n, s):
        copy = to_pair(i, h, n, s)
        pl.when(mid)(copy.start)
        waits.append((mid, copy))

    def outward(h):
        copy = to_mid(3, h, 1)

        @pl.when(mid)
        def _():
            line_in(3, h)
            copy.start()

        waits.append((mid, copy))

    def cross_sides(i):
        cross(i, 1, gx, slot(i))
        cross(i, 2, gy, slot(i))

    for h in range(2):
        line_in(1, h)
        forward(1, h, 1, 1)
        direct(1, h)
        outward(h)
        sides_in(0, h)
    cross_sides(0)
    cross(1, 0, dp, slot(1))
    gate_in_line(1)
    send_if(mid, gates.at[slot(1), k], gates.at[slot(1), k], ep_s.at[1], ez_r.at[1], pair)
    gate_line_3 = make(gates.at[slot(3), k], gates.at[slot(3), k], em_s.at[1], ez_r.at[1], across)

    @pl.when(mid)
    def _():
        got(gates.at[slot(3), k], ep_s.at[0], ez_r.at[2])
        gate_line_3.start()

    waits.append((mid, gate_line_3))
    for i, g in enumerate((gx, gy, gd)):
        got(picks_of.at[g], es.at[i], er.at[i])
    load_in.wait()
    gate_ready(0)
    absorb(from_own(0))
    line_in(2, 0)
    forward(2, 0, 2, 2)
    direct(2, 0, None, (0,))
    direct(2, 0, edge, (1,))
    sides_in(1, 0)
    relay(0, None, (0,))
    absorb(from_x(0))
    line_in(2, 1)
    forward(2, 1, 2, 2)
    direct(2, 0, mid, (1,))
    gate_in_line(2)
    send_if(mid, gates.at[slot(2), k], gates.at[slot(2), k], ep_s.at[2], ez_r.at[2], pair)
    sides_in(1, 1)
    relay(0, None, (1,))
    direct(2, 1)
    relay(1, edge)
    cross_sides(1)
    cross(2, 0, dp, slot(2))
    gate_ready(1)
    absorb(from_y(0))
    sides_in(2, 0)
    relay(1, mid)
    direct(3, 0, mid)
    direct(3, 1, mid)

    @pl.when(edge)
    def _():
        line_in(3, 0)
        direct(3, 0, True)

    absorb(from_own(1), from_x(1))

    @pl.when(edge)
    def _():
        got(gates.at[slot(3), k], ep_s.at[0], ez_r.at[2])

    send(gates.at[slot(3), k], gates.at[slot(3), k], eds.at[3], edr.at[3], partner)
    corner_in(0)

    @pl.when(edge)
    def _():
        line_in(3, 1)
        direct(3, 1, True)

    cross(3, 0, dp, slot(3))
    gate_ready(2)
    absorb(from_y(1), from_own(2))
    sides_in(2, 1)
    cross_sides(2)
    gate_ready(3)
    absorb(from_turned(0))
    absorb(from_x(2))
    passed_in(0, 0)
    absorb(from_y(2))
    corner_in(1)
    passed_in(0, 1)
    cross(2, 3, gd, passed(0))
    absorb(from_own(3))
    sides_in(3, 0)
    cross_half(0, 0, gx, slot(3))
    cross_half(1, 0, gy, slot(3))
    absorb(from_turned(1), from_passed(0))
    for n in range(2 * depth):
        for d in range(2):
            waits.append((None, make(own.at[rows[0]], own.at[rows[0]], xy_s.at[n // 2, d, n % 2], xy_r.at[0, 0, 0], side[d])))
    for n in range(4):
        waits.append((None, make(own.at[rows[0]], own.at[rows[0]], relay_s.at[n // 2, n % 2], relay_r.at[0, 0], side[0])))

    def accumulate_half(g, zz, h):
        lanes = slice(h * half, h * half + half)
        total, score = pre[g, rows[h]], logit[g, :, lanes]
        for kk in range(2):
            strip = pl.ds(pl.multiple_of((zz * 2 + kk) * width, width), width)
            block = xs[g, zz, kk, rows[h]]
            total += jnp.dot(block, win[strip, :], preferred_element_type=F32)
            score += lax.dot_general(gates[zz, kk], block, (((1,), (1,)), ((), ())), preferred_element_type=F32)
        pre[g, rows[h]] = total
        logit[g, :, lanes] = score

    def activate(g, h):
        lanes = slice(h * half, h * half + half)
        score = logit[g, :, lanes]
        row = lax.broadcasted_iota(jnp.int32, score.shape, 0)
        raised = jnp.where(row < experts, jnp.exp(score), 0.0)
        chance = raised / jnp.sum(raised, axis=0, keepdims=True)
        local = jnp.sum(jnp.where(row == dp, chance, 0.0), axis=0, keepdims=True)
        picks = picks_of[g, :, lanes].astype(F32)
        named = jnp.logical_and(jnp.logical_or(row == experts, row == experts + 1), picks == dp.astype(F32))
        hit = jnp.sum(jnp.where(named, 1.0, 0.0), axis=0, keepdims=True)
        scale = local.astype(BF16).astype(F32) * hit
        column = jnp.transpose(jnp.broadcast_to(scale, (128, half)))[:, :1]
        acted = jax.nn.gelu(pre[g, rows[h]], approximate=True)
        hidden[g, rows[h]] = (acted * column).astype(BF16)

    def product(g, zz, kk):
        cols = pl.ds(pl.multiple_of((zz * 2 + kk) * width, width), width)
        return jnp.dot(hidden[g], wout[:, cols], preferred_element_type=F32)

    order = [
        (gx, slot(3)), (gy, slot(3)), (gd, passed(1)),
        (gx, slot(2)), (gy, slot(2)), (gd, passed(0)), (gd, turned(1)),
        (gd, turned(0)), (dp, slot(3)),
        (gx, slot(1)), (gy, slot(1)),
        (dp, slot(2)), (dp, slot(1)),
        (gx, slot(0)), (gy, slot(0)), (dp, slot(0)),
    ]

    def lend(n, g, zz):
        give[zz, g] = product(g, zz, 1 - k).astype(BF16)
        make(give.at[zz, g], take.at[zz, g], ps.at[n], pr.at[n], partner).start()

    def keep(g, zz):
        part[zz, g] = (product(g, zz, k) + take[zz, g].astype(F32)).astype(BF16)

    def half_product(g, zz, kk, h):
        cols = pl.ds(pl.multiple_of((zz * 2 + kk) * width, width), width)
        return jnp.dot(hidden[g, rows[h]], wout[:, cols], preferred_element_type=F32)

    def lend_half(n, h):
        g, zz = order[n]
        give[zz, g, rows[h]] = half_product(g, zz, 1 - k, h).astype(BF16)
        send(give.at[zz, g, rows[h]], take.at[zz, g, rows[h]], ths.at[n, h], thr.at[n, h], partner)

    def keep_half(n, h):
        g, zz = order[n]
        got(take.at[zz, g, rows[h]], ths.at[n, h], thr.at[n, h])
        part[zz, g, rows[h]] = (half_product(g, zz, k, h) + take[zz, g, rows[h]].astype(F32)).astype(BF16)

    def two(ref, h):
        return jnp.concatenate([ref[gx, rows[h]], ref[gy, rows[h]]], axis=0)

    def ready_two(h):
        zz = slot(3)
        for n, g in enumerate((gx, gy)):
            got(xs.at[g, zz, 1 - k, rows[h]], hs.at[n, h], hr.at[n, h])
        lanes = slice(h * half, h * half + half)
        total = two(pre, h)
        score = jnp.concatenate([logit[gx, :, lanes], logit[gy, :, lanes]], axis=1)
        for kk in range(2):
            strip = pl.ds(pl.multiple_of((zz * 2 + kk) * width, width), width)
            block = jnp.concatenate([xs[gx, zz, kk, rows[h]], xs[gy, zz, kk, rows[h]]], axis=0)
            total += jnp.dot(block, win[strip, :], preferred_element_type=F32)
            score += lax.dot_general(gates[zz, kk], block, (((1,), (1,)), ((), ())), preferred_element_type=F32)
        for n, g in enumerate((gx, gy)):
            pre[g, rows[h]] = total[n * half:(n + 1) * half]
            logit[g, :, lanes] = score[:, n * half:(n + 1) * half]
            activate(g, h)
        cols = pl.ds(pl.multiple_of((zz * 2 + 1 - k) * width, width), width)
        lent = jnp.dot(two(hidden, h), wout[:, cols], preferred_element_type=F32).astype(BF16)
        for n, g in enumerate((gx, gy)):
            give[zz, g, rows[h]] = lent[n * half:(n + 1) * half]
            send(give.at[zz, g, rows[h]], take.at[zz, g, rows[h]], ths.at[n, h], thr.at[n, h], partner)

    def keep_two(h):
        zz = slot(3)
        cols = pl.ds(pl.multiple_of((zz * 2 + k) * width, width), width)
        kept = jnp.dot(two(hidden, h), wout[:, cols], preferred_element_type=F32)
        for n, g in enumerate((gx, gy)):
            got(take.at[zz, g, rows[h]], ths.at[n, h], thr.at[n, h])
            summed = kept[n * half:(n + 1) * half] + take[zz, g, rows[h]].astype(F32)
            part[zz, g, rows[h]] = summed.astype(BF16)
            to_side(3, n, h)

    def ready(n, h):
        g, zz = order[n]
        got(xs.at[g, zz, 1 - k, rows[h]], hs.at[n, h], hr.at[n, h])
        accumulate_half(g, zz, h)
        activate(g, h)
        lend_half(n, h)

    def lend_all(lo, hi):
        gs, zs = [w[0] for w in order[lo:hi]], [w[1] for w in order[lo:hi]]
        several(hi - lo, lambda c: lend(lo + c, choose(c, gs), choose(c, zs)))

    def taken(n):
        g, zz = order[n]
        got(take.at[zz, g], ps.at[n], pr.at[n])

    def keep_all(lo, hi):
        for n in range(lo, hi):
            taken(n)
        gs, zs = [w[0] for w in order[lo:hi]], [w[1] for w in order[lo:hi]]
        several(hi - lo, lambda c: keep(choose(c, gs), choose(c, zs)))

    for n in range(3, len(order)):
        g, zz = order[n]
        waits.append((None, make(give.at[zz, g], take.at[zz, g], ps.at[n], pr.at[n], partner)))

    def to_side(i, d, h):
        g = (gx, gy)[d]
        send(part.at[slot(i), g, rows[h]], from_side.at[i, d, h], side_s.at[i, d, h], side_r.at[i, d, h], side[d])

    def to_pair_passed(j, h):
        zz = passed(j)
        send(part.at[zz, gd, rows[h]], from_pair.at[j, h], pair_s.at[j, h], pair_r.at[j, h], pair)

    def to_corner(j, h):
        zz = turned(j)
        got(from_pair.at[j, h], pair_s.at[j, h], pair_r.at[j, h])
        part[zz, gd, rows[h]] = (part[zz, gd, rows[h]].astype(F32) + from_pair[j, h].astype(F32)).astype(BF16)
        send(part.at[zz, gd, rows[h]], from_corner.at[j, h], corner_s.at[j, h], corner_r.at[j, h], side[h])

    def corner_add(j):
        zz = turned(j)
        for h, g in ((0, gy), (1, gx)):
            got(from_corner.at[j, h], corner_s.at[j, h], corner_r.at[j, h])
            part[zz, g, rows[h]] = (part[zz, g, rows[h]].astype(F32) + from_corner[j, h].astype(F32)).astype(BF16)

    def gathered(i, h):
        total = part[slot(i), dp, rows[h]].astype(F32)
        for d in range(2):
            got(from_side.at[i, d, h], side_s.at[i, d, h], side_r.at[i, d, h])
            total += from_side[i, d, h].astype(F32)
        return total

    def line_pair_in(n, h):
        got(line_pair.at[n, h], lp_s.at[0, h], lp_r.at[n, h])
        return line_pair[n, h].astype(F32)

    def line_mid_in(n, h):
        got(line_mid.at[n, h], lm_s.at[0, h], lm_r.at[n, h])
        return line_mid[n, h].astype(F32)

    def line_to_pair(i, h, n):
        return make(part.at[slot(i), dp, rows[h]], line_pair.at[n, h], lp_s.at[n, h], lp_r.at[n, h], pair)

    def line_to_mid(i, h, n):
        return make(part.at[slot(i), dp, rows[h]], line_mid.at[n, h], lm_s.at[n, h], lm_r.at[n, h], across)

    def settle(i, h):
        total = gathered(i, h)
        zz = slot(i)
        to_pair_copy = line_to_pair(i, h, i - 1)

        @pl.when(edge)
        def _():
            part[zz, dp, rows[h]] = total.astype(BF16)
            to_pair_copy.start()

        waits.append((edge, to_pair_copy))
        if i == 3:

            @pl.when(mid)
            def _():
                part[zz, dp, rows[h]] = total.astype(BF16)
        else:
            copy = line_to_mid(i, h, 2 - i)

            @pl.when(mid)
            def _():
                part[zz, dp, rows[h]] = (total + line_pair_in(i, h)).astype(BF16)
                copy.start()

            waits.append((mid, copy))

    def outer(h):
        copy = line_to_pair(3, h, 0)

        @pl.when(mid)
        def _():
            zz = slot(3)
            came = line_mid_in(0, h)
            part[zz, dp, rows[h]] = (part[zz, dp, rows[h]].astype(F32) + came).astype(BF16)
            copy.start()

        waits.append((mid, copy))

    load_out.wait()
    ready_two(0)
    passed_in(1, 0)
    cross_half(2, 0, gd, passed(1))
    sides_in(3, 1)
    cross_half(0, 1, gx, slot(3))
    cross_half(1, 1, gy, slot(3))
    ready(2, 0)
    keep_two(0)
    passed_in(1, 1)
    cross_half(2, 1, gd, passed(1))
    ready_two(1)
    keep_half(2, 0)
    to_pair_passed(1, 0)
    ready(2, 1)
    keep_two(1)
    lend_all(3, 5)
    keep_half(2, 1)
    to_pair_passed(1, 1)
    lend_all(5, 7)
    keep_all(3, 5)
    to_side(2, 0, 0)
    to_side(2, 1, 1)
    keep_all(5, 7)
    to_pair_passed(0, 0)
    to_pair_passed(0, 1)
    to_corner(1, 0)
    activate(dp, 0)
    activate(dp, 1)
    lend_all(7, 9)
    to_corner(1, 1)
    lend_all(9, 11)
    keep_all(7, 9)
    settle(3, 0)
    settle(3, 1)
    lend_all(11, 13)
    to_corner(0, 0)
    keep_all(9, 11)
    pl.when(mid)(functools.partial(corner_add, 1))
    to_side(2, 1, 0)
    to_side(2, 0, 1)
    to_corner(0, 1)
    pl.when(edge)(functools.partial(corner_add, 1))
    to_side(1, 0, 0)
    lend_all(13, 16)
    keep_all(11, 13)
    pl.when(mid)(functools.partial(corner_add, 0))
    to_side(1, 1, 0)
    to_side(1, 0, 1)
    to_side(1, 1, 1)
    keep_all(13, 16)
    pl.when(edge)(functools.partial(corner_add, 0))
    for h in range(2):
        to_side(0, 0, h)
        to_side(0, 1, h)
    settle(2, 0)
    settle(2, 1)
    outer(0)
    settle(1, 0)
    settle(1, 1)
    outer(1)
    for h in range(2):
        total = gathered(0, h)

        @pl.when(mid)
        def _():
            out[rows[h]] = (total + line_pair_in(0, h) + line_mid_in(1, h)).astype(BF16)

        @pl.when(edge)
        def _():
            out[rows[h]] = (total + line_pair_in(0, h)).astype(BF16)

    for role, copy in waits:
        if role is None:
            copy.wait_send()
        else:
            pl.when(role)(copy.wait_send)


def tokens_plan(tokens, routing, gate_weight, expert_in, expert_out):
    group, width = tokens.shape
    depth = lax.axis_size("expert") // 2
    experts = gate_weight.shape[1]
    model, inner = expert_in.shape[1:]
    half = group // 2
    vmem = pltpu.VMEM
    dma = pltpu.SemaphoreType.DMA
    return pl.pallas_call(
        functools.partial(whole_kernel, experts),
        out_shape=jax.ShapeDtypeStruct((group, width), BF16),
        in_specs=[pl.BlockSpec(memory_space=pl.ANY)] * 5,
        out_specs=pl.BlockSpec(memory_space=vmem),
        scratch_shapes=[
            vmem((8, width), BF16),
            vmem((experts, width), BF16),
            vmem((2, group), jnp.int32),
            vmem((4, depth, 2, group, width), BF16),
            vmem((depth, 2, 8, width), BF16),
            vmem((4, 8, width), BF16),
            vmem((model, inner), BF16),
            vmem((inner, model), BF16),
            vmem((4, group, inner), F32),
            vmem((4, 8, group), F32),
            vmem((4, group, inner), BF16),
            vmem((depth, 4, group, width), BF16),
            vmem((depth, 4, group, width), BF16),
            vmem((depth, 4, group, width), BF16),
            vmem((depth, 2, 2, half, width), BF16),
            vmem((2, 2, half, width), BF16),
            vmem((2, 2, half, width), BF16),
            vmem((3, 2, half, width), BF16),
            vmem((2, 2, half, width), BF16),
            dma((5,)),
            dma((depth, 2, 2)), dma((depth, 2, 2)),
            dma((2, 2)), dma((2, 2)),
            dma((3, 2)), dma((2, 2)), dma((3, 2)),
            dma((2, 2)), dma((2, 2)),
            dma((depth, 4)), dma((depth, 4)),
            dma((3,)), dma((3,)),
            dma((3,)), dma((2,)), dma((3,)),
            dma((depth,)), dma((depth,)),
            dma((4 * depth,)), dma((4 * depth,)),
            dma((3, 2)), dma((3, 2)), dma((3, 2)), dma((3, 2)),
            dma((depth, 2, 2)), dma((depth, 2, 2)),
            dma((2, 2)), dma((2, 2)),
            dma((2, 2)), dma((2, 2)),
            dma((3, 2)), dma((3, 2)),
            dma((2, 2)), dma((2, 2)),
        ],
        compiler_params=pltpu.CompilerParams(
            collective_id=0, has_side_effects=True, vmem_limit_bytes=63 * 1024 * 1024
        ),
    )(tokens, gate_weight.T, routing.T, expert_in, expert_out)


def solution(mesh):
    placed = (
        P("dp", "expert"),
        P("dp", None),
        P("expert", None),
        P("dp", None, "expert"),
        P("dp", "expert", None),
    )
    body = tokens_plan if tuple(mesh.shape.values()) == (4, 8) else slots_plan
    return jax.shard_map(
        body, mesh=mesh, in_specs=placed, out_specs=P("dp", "expert"), check_vma=False
    )
```

```python
import functools

import jax
import jax.numpy as jnp
from jax import lax
from jax.experimental import pallas as pl
from jax.experimental.pallas import tpu as pltpu
from jax.sharding import PartitionSpec as P


def softmax_rows(logits):
    raised = jnp.exp(logits)
    return raised / jnp.sum(raised, axis=-1, keepdims=True)


def pick_chosen(softmax_all, picks):
    experts = softmax_all.shape[1]
    labels = lax.broadcasted_iota(jnp.int32, (picks.shape[0], 2, experts), 2)
    selected = labels == picks[:, :, None]
    return jnp.sum(jnp.where(selected, softmax_all[:, None, :], 0.0), axis=-1).astype(jnp.bfloat16)


def expert_rows(block_rows, weight_in, weight_out):
    sources = block_rows.shape[0]
    slots_here = block_rows.shape[1]
    width_local = block_rows.shape[2]
    flat_rows = block_rows.reshape(sources * slots_here, width_local)
    pre_act = jnp.dot(
        lax.all_gather(flat_rows, "expert", axis=1, tiled=True),
        weight_in,
        preferred_element_type=jnp.float32,
    )
    hidden = jax.nn.gelu(pre_act, approximate=True).astype(jnp.bfloat16)
    partial_out = jnp.dot(hidden, weight_out, preferred_element_type=jnp.float32)
    summed = lax.psum_scatter(
        partial_out.astype(jnp.bfloat16), "expert", scatter_dimension=1, tiled=True
    )
    return summed.reshape(sources, slots_here, width_local)


def slots_plan(tokens, routing, gate_weight, expert_in, expert_out):
    group_size = tokens.shape[0]
    width_local = tokens.shape[1]
    experts = gate_weight.shape[1]
    dp_count = lax.axis_size("dp")
    capacity = 3 * group_size // dp_count
    weight_in = expert_in[0]
    weight_out = expert_out[0]
    partial_logits = jnp.dot(tokens, gate_weight, preferred_element_type=jnp.float32)
    logits = lax.psum(partial_logits, "expert")
    chosen = pick_chosen(softmax_rows(logits), routing)
    order = jnp.concatenate([routing[:, 0], routing[:, 1]], axis=0)
    labels = lax.broadcasted_iota(jnp.int32, (2 * group_size, experts), 1)
    onehot = (labels == order[:, None]).astype(jnp.int32)
    before = jnp.cumsum(onehot, axis=0) - onehot
    slot_flat = jnp.sum(before * onehot, axis=1)
    slot_index = jnp.stack([slot_flat[:group_size], slot_flat[group_size:]], axis=1)
    target = routing * capacity + slot_index
    columns = lax.broadcasted_iota(jnp.int32, (group_size, experts * capacity), 1)
    first_hit = columns == target[:, 0:1]
    second_hit = columns == target[:, 1:2]
    assign = jnp.logical_or(first_hit, second_hit).astype(jnp.bfloat16)
    outgoing = jnp.einsum("gs,gd->sd", assign, tokens, preferred_element_type=jnp.float32)
    outgoing = outgoing.astype(jnp.bfloat16).reshape(experts, capacity, width_local)
    incoming = lax.all_to_all(outgoing, "dp", split_axis=0, concat_axis=0, tiled=True)
    processed = expert_rows(incoming, weight_in, weight_out)
    returned_rows = lax.all_to_all(processed, "dp", split_axis=0, concat_axis=0, tiled=True)
    zero_weight = jnp.zeros((), jnp.bfloat16)
    combine = jnp.where(first_hit, chosen[:, 0:1], zero_weight) + jnp.where(
        second_hit, chosen[:, 1:2], zero_weight
    )
    mixed = jnp.dot(
        combine,
        returned_rows.reshape(experts * capacity, width_local),
        preferred_element_type=jnp.float32,
    )
    return mixed.astype(jnp.bfloat16)


MESH = pl.DeviceIdType.MESH
F32 = jnp.float32
BF16 = jnp.bfloat16


def whole_kernel(
    experts,
    tok_hbm, gate_hbm, routes_hbm, win_hbm, wout_hbm, out,
    extra, gate_in, routes,
    xs, gates, picks_of, win, wout, pre, logit, hidden, give, take, part,
    from_side, from_corner, from_pair, line_pair, line_mid,
    wsem, xy_s, xy_r, relay_s, relay_r, zp_s, zm_s, z_r, pass_s, pass_r, ds, dr,
    es, er, ep_s, em_s, ez_r, eds, edr,
    ps, pr, hs, hr, ths, thr, side_s, side_r, corner_s, corner_r, pair_s, pair_r, lp_s, lp_r, lm_s, lm_r, far_s, far_r, end_s, end_r,
):
    dp, me = lax.axis_index("dp"), lax.axis_index("expert")
    z, k = me // 2, me % 2
    depth = lax.axis_size("expert") // 2
    group, width = tok_hbm.shape
    half = group // 2
    gx, gy = dp // 2 * 2 + 1 - dp % 2, (1 - dp // 2) * 2 + dp % 2
    gd = 3 - dp
    upper = z // 2
    near = z * (1 - upper) + (depth - 1 - z) * upper
    mid, edge = near == 1, near == 0
    rows = (pl.ds(0, half), pl.ds(half, half))
    partner = (dp, z * 2 + 1 - k)

    def at(q):
        return q * (1 - upper) + (depth - 1 - q) * upper

    def slot(i):
        return at(lax.rem(near + i, depth))

    def turned(j):
        return at(j + 2 * near)

    def passed(j):
        return at(j + 2 * (1 - near))

    pair, across = (dp, at(1 - near) * 2 + k), (dp, (depth - 1 - z) * 2 + k)
    side = ((gx, me), (gy, me))
    waits, late = [], []

    def make(src, dst, s_sem, r_sem, who):
        return pltpu.make_async_remote_copy(src, dst, s_sem, r_sem, device_id=who, device_id_type=MESH)

    def send(src, dst, s_sem, r_sem, who):
        copy = make(src, dst, s_sem, r_sem, who)
        copy.start()
        waits.append((None, copy))

    def send_if(role, src, dst, s_sem, r_sem, who):
        copy = make(src, dst, s_sem, r_sem, who)
        pl.when(role)(copy.start)
        waits.append((role, copy))

    def drain(copies):
        for copy in [c for role, c in copies if role is None]:
            copy.wait_send()
        for which in (edge, mid):

            @pl.when(which)
            def _():
                for copy in [c for role, c in copies if role is which]:
                    copy.wait_send()

    def got(ref, s_sem, r_sem):
        make(ref, ref, s_sem, r_sem, partner).wait_recv()

    own = xs.at[dp, z, k]
    small = [
        pltpu.make_async_copy(src, dst, wsem.at[2 + i])
        for i, (src, dst) in enumerate(((tok_hbm, own), (gate_hbm, gate_in), (routes_hbm, routes)))
    ]
    load_in = pltpu.make_async_copy(win_hbm.at[0], win, wsem.at[0])
    load_out = pltpu.make_async_copy(wout_hbm.at[0], wout, wsem.at[1])
    barrier = pltpu.get_barrier_semaphore()
    for who in (partner, *side, (gd, me), pair):
        pl.semaphore_signal(barrier, inc=1, device_id=who, device_id_type=MESH)

    @pl.when(mid)
    def _():
        pl.semaphore_signal(barrier, inc=1, device_id=across, device_id_type=MESH)

    for copy in (*small, load_in, load_out):
        copy.start()
    pl.semaphore_wait(barrier, 5 + near)
    small[0].wait()

    def mine(i):
        return own if i == 0 else xs.at[dp, slot(i), k]

    def span(h):
        return pl.ds(pl.multiple_of(h * half, half), half)

    def turn(i, d, h):
        return h + near * (1 - 2 * h) if i == 2 and d == 1 else h

    def direct(i, h, role=None, ways=(0, 1)):
        for d in ways:
            hh = turn(i, d, h)
            copy = make(
                mine(i).at[span(hh)], xs.at[dp, slot(i), k, span(hh)], xy_s.at[i, d, hh], xy_r.at[i, d, hh], side[d]
            )
            if role is None:
                copy.start()
            else:
                pl.when(role)(copy.start)

    def to_pair(i, h, n, s):
        zz = slot(i)
        return make(mine(i).at[rows[h]], xs.at[dp, zz, k, rows[h]], zp_s.at[n, h], z_r.at[s, h], pair)

    def to_mid(i, h, n):
        zz = slot(i)
        return make(mine(i).at[rows[h]], xs.at[dp, zz, k, rows[h]], zm_s.at[n, h], z_r.at[n, h], across)

    def line_in(i, h):
        got(xs.at[dp, slot(i), k, rows[h]], zp_s.at[0, h], z_r.at[i - 1, h])

    def cross(i, t, g, zz):
        block = xs.at[g, zz, k]
        send(block, xs.at[g, zz, k], ds.at[i, t], dr.at[i, t], partner)

    def crossed(i, t, g, zz):
        got(xs.at[g, zz, 1 - k], ds.at[i, t], dr.at[i, t])

    def cross_half(n, h, g, zz):
        block = xs.at[g, zz, k, rows[h]]
        send(block, block, hs.at[n, h], hr.at[n, h], partner)

    def sides_in(i, h):
        for d, g in enumerate((gx, gy)):
            hh = turn(i, d, h)
            got(xs.at[g, slot(i), k, span(hh)], xy_s.at[i, d, hh], xy_r.at[i, d, hh])

    def relay(j, role=None, ways=(0, 1)):
        zz = turned(j)
        for n in ways:
            g, who = ((gx, side[1]), (gy, side[0]))[n]
            block = xs.at[g, zz, k, rows[n]]
            copy = make(block, block, relay_s.at[j, n], relay_r.at[j, n], who)
            if role is None:
                copy.start()
            else:
                pl.when(role)(copy.start)

    def corner_in(j):
        zz = turned(j)
        for h in range(2):
            block = xs.at[gd, zz, k, rows[h]]
            got(block, relay_s.at[j, h], relay_r.at[j, h])
            send(block, block, pass_s.at[j, h], pass_r.at[j, h], pair)
        cross(j, 3, gd, zz)

    def passed_in(j, h):
        got(xs.at[gd, passed(j), k, rows[h]], pass_s.at[j, h], pass_r.at[j, h])

    own_line = 2 - 2 * near
    for h in range(2):
        first = to_pair(0, h, 0, own_line)
        first.start()
        waits.append((None, first))
        second = to_mid(0, h, 0)
        pl.when(mid)(second.start)
        waits.append((mid, second))
        direct(0, h)
    cross(0, 0, dp, z)

    small[1].wait()
    small[2].wait()
    wide = lax.broadcasted_iota(jnp.int32, (8, experts), 0) == lax.broadcasted_iota(jnp.int32, (8, experts), 1)
    both = lax.broadcasted_iota(jnp.int32, (8, 2), 0) == lax.broadcasted_iota(jnp.int32, (8, 2), 1) + experts
    gate_rows = jnp.dot(jnp.where(wide, 1.0, 0.0).astype(BF16), gate_in[...], preferred_element_type=F32)
    route_rows = jnp.dot(
        jnp.where(both, 1.0, 0.0).astype(BF16), routes[...].astype(F32).astype(BF16), preferred_element_type=F32
    )
    extra[...] = gate_rows.astype(BF16)
    extra[:, :group] = (gate_rows[:, :group] + route_rows).astype(BF16)
    for i, who in enumerate((*side, (gd, me))):
        send(extra, picks_of.at[dp], es.at[i], er.at[i], who)
    send(extra, gates.at[z, k], ep_s.at[0], ez_r.at[own_line], pair)
    send_if(mid, extra, gates.at[z, k], em_s.at[0], ez_r.at[0], across)
    send(extra, gates.at[z, k], eds.at[0], edr.at[0], partner)
    picks_of[dp] = extra[...]
    gates[z, k] = extra[...]
    pre[...] = jnp.zeros_like(pre)
    logit[...] = jnp.zeros_like(logit)

    def gate_in_line(i):
        zz = slot(i)
        got(gates.at[zz, k], ep_s.at[0], ez_r.at[i - 1])
        send(gates.at[zz, k], gates.at[zz, k], eds.at[i], edr.at[i], partner)

    def gate_ready(i):
        got(gates.at[slot(i), 1 - k], eds.at[i], edr.at[i])

    def accumulate(g, zz):
        total, score = pre[g], logit[g]
        for kk in range(2):
            strip = pl.ds(pl.multiple_of((zz * 2 + kk) * width, width), width)
            block = xs[g, zz, kk]
            total += jnp.dot(block, win[strip, :], preferred_element_type=F32)
            score += lax.dot_general(gates[zz, kk], block, (((1,), (1,)), ((), ())), preferred_element_type=F32)
        pre[g] = total
        logit[g] = score

    def choose(c, options):
        chosen = options[-1]
        for n in range(len(options) - 2, -1, -1):
            chosen = jnp.where(c == n, options[n], chosen)
        return chosen

    def several(count, fn):
        lax.fori_loop(0, count, lambda c, carry: fn(c) or carry, 0)

    def absorb(*which):
        for i, t, g, zz in which:
            crossed(i, t, g, zz)
        gs, zs = [w[2] for w in which], [w[3] for w in which]
        several(len(which), lambda c: accumulate(choose(c, gs), choose(c, zs)))

    def from_own(i):
        return (i, 0, dp, slot(i))

    def from_x(i):
        return (i, 1, gx, slot(i))

    def from_y(i):
        return (i, 2, gy, slot(i))

    def from_turned(j):
        return (j, 3, gd, turned(j))

    def from_passed(j):
        return (2 + j, 3, gd, passed(j))

    def forward(i, h, n, s):
        copy = to_pair(i, h, n, s)
        pl.when(mid)(copy.start)
        waits.append((mid, copy))

    def outward(h):
        copy = to_mid(3, h, 1)

        @pl.when(mid)
        def _():
            line_in(3, h)
            copy.start()

        waits.append((mid, copy))

    def cross_sides(i):
        cross(i, 1, gx, slot(i))
        cross(i, 2, gy, slot(i))

    for h in range(2):
        line_in(1, h)
        forward(1, h, 1, 1)
        direct(1, h)
        outward(h)
        sides_in(0, h)
    cross_sides(0)
    cross(1, 0, dp, slot(1))
    gate_in_line(1)
    send_if(mid, gates.at[slot(1), k], gates.at[slot(1), k], ep_s.at[1], ez_r.at[1], pair)
    gate_line_3 = make(gates.at[slot(3), k], gates.at[slot(3), k], em_s.at[1], ez_r.at[1], across)

    @pl.when(mid)
    def _():
        got(gates.at[slot(3), k], ep_s.at[0], ez_r.at[2])
        gate_line_3.start()

    waits.append((mid, gate_line_3))
    for i, g in enumerate((gx, gy, gd)):
        got(picks_of.at[g], es.at[i], er.at[i])
    load_in.wait()
    gate_ready(0)
    absorb(from_own(0))
    line_in(2, 0)
    forward(2, 0, 2, 2)
    direct(2, 0, None, (0,))
    direct(2, 0, edge, (1,))
    sides_in(1, 0)
    relay(0, None, (0,))
    absorb(from_x(0))
    line_in(2, 1)
    forward(2, 1, 2, 2)
    direct(2, 0, mid, (1,))
    gate_in_line(2)
    send_if(mid, gates.at[slot(2), k], gates.at[slot(2), k], ep_s.at[2], ez_r.at[2], pair)
    sides_in(1, 1)
    relay(0, None, (1,))
    direct(2, 1)
    relay(1, edge)
    cross_sides(1)
    cross(2, 0, dp, slot(2))
    gate_ready(1)
    absorb(from_y(0))
    sides_in(2, 0)
    relay(1, mid)
    direct(3, 0, mid)
    direct(3, 1, mid)

    @pl.when(edge)
    def _():
        line_in(3, 0)
        direct(3, 0, True)

    absorb(from_own(1), from_x(1))

    @pl.when(edge)
    def _():
        got(gates.at[slot(3), k], ep_s.at[0], ez_r.at[2])

    send(gates.at[slot(3), k], gates.at[slot(3), k], eds.at[3], edr.at[3], partner)
    corner_in(0)

    @pl.when(edge)
    def _():
        line_in(3, 1)
        direct(3, 1, True)

    cross(3, 0, dp, slot(3))
    gate_ready(2)
    absorb(from_y(1), from_own(2))
    sides_in(2, 1)
    cross_sides(2)
    gate_ready(3)
    absorb(from_turned(0))
    absorb(from_x(2))
    passed_in(0, 0)
    absorb(from_y(2))
    corner_in(1)
    passed_in(0, 1)
    cross(2, 3, gd, passed(0))
    absorb(from_own(3))
    sides_in(3, 0)
    cross_half(0, 0, gx, slot(3))
    cross_half(1, 0, gy, slot(3))
    absorb(from_turned(1))
    for n in range(2 * depth):
        for d in range(2):
            waits.append((None, make(own.at[rows[0]], own.at[rows[0]], xy_s.at[n // 2, d, n % 2], xy_r.at[0, 0, 0], side[d])))
    for n in range(4):
        waits.append((None, make(own.at[rows[0]], own.at[rows[0]], relay_s.at[n // 2, n % 2], relay_r.at[0, 0], side[0])))

    def accumulate_half(g, zz, h):
        lanes = slice(h * half, h * half + half)
        total, score = pre[g, rows[h]], logit[g, :, lanes]
        for kk in range(2):
            strip = pl.ds(pl.multiple_of((zz * 2 + kk) * width, width), width)
            block = xs[g, zz, kk, rows[h]]
            total += jnp.dot(block, win[strip, :], preferred_element_type=F32)
            score += lax.dot_general(gates[zz, kk], block, (((1,), (1,)), ((), ())), preferred_element_type=F32)
        pre[g, rows[h]] = total
        logit[g, :, lanes] = score

    def activate(g, h):
        lanes = slice(h * half, h * half + half)
        score = logit[g, :, lanes]
        row = lax.broadcasted_iota(jnp.int32, score.shape, 0)
        raised = jnp.where(row < experts, jnp.exp(score), 0.0)
        chance = raised / jnp.sum(raised, axis=0, keepdims=True)
        local = jnp.sum(jnp.where(row == dp, chance, 0.0), axis=0, keepdims=True)
        picks = picks_of[g, :, lanes].astype(F32)
        named = jnp.logical_and(jnp.logical_or(row == experts, row == experts + 1), picks == dp.astype(F32))
        hit = jnp.sum(jnp.where(named, 1.0, 0.0), axis=0, keepdims=True)
        scale = local.astype(BF16).astype(F32) * hit
        column = jnp.transpose(jnp.broadcast_to(scale, (128, half)))[:, :1]
        acted = jax.nn.gelu(pre[g, rows[h]], approximate=True)
        hidden[g, rows[h]] = (acted * column).astype(BF16)

    def product(g, zz, kk):
        cols = pl.ds(pl.multiple_of((zz * 2 + kk) * width, width), width)
        return jnp.dot(hidden[g], wout[:, cols], preferred_element_type=F32)

    order = [
        (gx, slot(3)), (gy, slot(3)), (gd, passed(1)),
        (gx, slot(2)), (gy, slot(2)), (gd, passed(0)), (gd, turned(1)),
        (gd, turned(0)), (dp, slot(3)),
        (gx, slot(1)), (gy, slot(1)),
        (dp, slot(2)), (dp, slot(1)),
        (gx, slot(0)), (gy, slot(0)), (dp, slot(0)),
    ]

    def lend(n, g, zz):
        give[zz, g] = product(g, zz, 1 - k).astype(BF16)
        make(give.at[zz, g], take.at[zz, g], ps.at[n], pr.at[n], partner).start()

    def keep(g, zz):
        part[zz, g] = (product(g, zz, k) + take[zz, g].astype(F32)).astype(BF16)

    def half_product(g, zz, kk, h):
        cols = pl.ds(pl.multiple_of((zz * 2 + kk) * width, width), width)
        return jnp.dot(hidden[g, rows[h]], wout[:, cols], preferred_element_type=F32)

    def lend_half(n, h):
        g, zz = order[n]
        give[zz, g, rows[h]] = half_product(g, zz, 1 - k, h).astype(BF16)
        send(give.at[zz, g, rows[h]], take.at[zz, g, rows[h]], ths.at[n, h], thr.at[n, h], partner)

    def keep_half(n, h):
        g, zz = order[n]
        got(take.at[zz, g, rows[h]], ths.at[n, h], thr.at[n, h])
        part[zz, g, rows[h]] = (half_product(g, zz, k, h) + take[zz, g, rows[h]].astype(F32)).astype(BF16)

    def two(ref, h):
        return jnp.concatenate([ref[gx, rows[h]], ref[gy, rows[h]]], axis=0)

    def ready_two(h):
        zz = slot(3)
        for n, g in enumerate((gx, gy)):
            got(xs.at[g, zz, 1 - k, rows[h]], hs.at[n, h], hr.at[n, h])
        lanes = slice(h * half, h * half + half)
        total = two(pre, h)
        score = jnp.concatenate([logit[gx, :, lanes], logit[gy, :, lanes]], axis=1)
        for kk in range(2):
            strip = pl.ds(pl.multiple_of((zz * 2 + kk) * width, width), width)
            block = jnp.concatenate([xs[gx, zz, kk, rows[h]], xs[gy, zz, kk, rows[h]]], axis=0)
            total += jnp.dot(block, win[strip, :], preferred_element_type=F32)
            score += lax.dot_general(gates[zz, kk], block, (((1,), (1,)), ((), ())), preferred_element_type=F32)
        for n, g in enumerate((gx, gy)):
            pre[g, rows[h]] = total[n * half:(n + 1) * half]
            logit[g, :, lanes] = score[:, n * half:(n + 1) * half]
            activate(g, h)
        cols = pl.ds(pl.multiple_of((zz * 2 + 1 - k) * width, width), width)
        lent = jnp.dot(two(hidden, h), wout[:, cols], preferred_element_type=F32).astype(BF16)
        for n, g in enumerate((gx, gy)):
            give[zz, g, rows[h]] = lent[n * half:(n + 1) * half]
            send(give.at[zz, g, rows[h]], take.at[zz, g, rows[h]], ths.at[n, h], thr.at[n, h], partner)

    def keep_two(h):
        zz = slot(3)
        cols = pl.ds(pl.multiple_of((zz * 2 + k) * width, width), width)
        kept = jnp.dot(two(hidden, h), wout[:, cols], preferred_element_type=F32)
        for n, g in enumerate((gx, gy)):
            got(take.at[zz, g, rows[h]], ths.at[n, h], thr.at[n, h])
            summed = kept[n * half:(n + 1) * half] + take[zz, g, rows[h]].astype(F32)
            part[zz, g, rows[h]] = summed.astype(BF16)
            to_side(3, n, h)

    def ready(n, h):
        g, zz = order[n]
        got(xs.at[g, zz, 1 - k, rows[h]], hs.at[n, h], hr.at[n, h])
        accumulate_half(g, zz, h)
        activate(g, h)
        lend_half(n, h)

    def lend_all(lo, hi):
        gs, zs = [w[0] for w in order[lo:hi]], [w[1] for w in order[lo:hi]]
        several(hi - lo, lambda c: lend(lo + c, choose(c, gs), choose(c, zs)))

    def taken(n):
        g, zz = order[n]
        got(take.at[zz, g], ps.at[n], pr.at[n])

    def keep_all(lo, hi):
        for n in range(lo, hi):
            taken(n)
        gs, zs = [w[0] for w in order[lo:hi]], [w[1] for w in order[lo:hi]]
        several(hi - lo, lambda c: keep(choose(c, gs), choose(c, zs)))

    for n in range(3, len(order)):
        g, zz = order[n]
        waits.append((None, make(give.at[zz, g], take.at[zz, g], ps.at[n], pr.at[n], partner)))

    def to_side(i, d, h):
        g = (gx, gy)[d]
        make(part.at[slot(i), g, rows[h]], from_side.at[i, d, h], side_s.at[i, d, h], side_r.at[i, d, h], side[d]).start()

    for n in range(4 * depth):
        i, d, h = n // 4, n // 2 % 2, n % 2
        kept = make(own.at[rows[0]], own.at[rows[0]], side_s.at[i, d, h], side_r.at[i, d, h], side[d])
        (late if i < 2 else waits).append((None, kept))

    def to_pair_passed(j, h):
        zz = passed(j)
        send(part.at[zz, gd, rows[h]], from_pair.at[j, h], pair_s.at[j, h], pair_r.at[j, h], pair)

    def to_corner(j, h):
        zz = turned(j)
        got(from_pair.at[j, h], pair_s.at[j, h], pair_r.at[j, h])
        part[zz, gd, rows[h]] = (part[zz, gd, rows[h]].astype(F32) + from_pair[j, h].astype(F32)).astype(BF16)
        send(part.at[zz, gd, rows[h]], from_corner.at[j, h], corner_s.at[j, h], corner_r.at[j, h], side[h])

    def corner_add(j, h):
        zz, g = turned(j), (gy, gx)[h]
        got(from_corner.at[j, h], corner_s.at[j, h], corner_r.at[j, h])
        part[zz, g, rows[h]] = (part[zz, g, rows[h]].astype(F32) + from_corner[j, h].astype(F32)).astype(BF16)

    def gathered(i, h):
        total = part[slot(i), dp, rows[h]].astype(F32)
        for d in range(2):
            got(from_side.at[i, d, h], side_s.at[i, d, h], side_r.at[i, d, h])
            total += from_side[i, d, h].astype(F32)
        return total

    def line_pair_in(n, h):
        got(line_pair.at[n, h], lp_s.at[0, h], lp_r.at[n, h])
        return line_pair[n, h].astype(F32)

    def line_mid_in(n, h):
        got(line_mid.at[n, h], lm_s.at[0, h], lm_r.at[n, h])
        return line_mid[n, h].astype(F32)

    def line_to_pair(i, h, n):
        return make(part.at[slot(i), dp, rows[h]], line_pair.at[n, h], lp_s.at[n, h], lp_r.at[n, h], pair)

    def line_to_mid(i, h, n):
        return make(part.at[slot(i), dp, rows[h]], line_mid.at[n, h], lm_s.at[n, h], lm_r.at[n, h], across)

    fine = half // 2

    def strip_of(h, c):
        return pl.ds(h * half + c * fine, fine)

    def far_to_mid(h, c):
        n = 2 * h + c
        piece = line_mid.at[0, h, pl.ds(c * fine, fine)]
        return make(part.at[slot(2), dp, strip_of(h, c)], piece, far_s.at[n], far_r.at[n], across)

    def far_to_edge(h, c):
        n = 2 * h + c
        piece = line_pair.at[0, h, pl.ds(c * fine, fine)]
        return make(part.at[slot(3), dp, strip_of(h, c)], piece, end_s.at[n], end_r.at[n], pair)

    def far_in(h, c):
        got(line_mid.at[0, h, pl.ds(c * fine, fine)], far_s.at[0], far_r.at[2 * h + c])

    def end_in(h, c):
        got(line_pair.at[0, h, pl.ds(c * fine, fine)], end_s.at[0], end_r.at[2 * h + c])

    def settle_edge(i, h):
        part[slot(i), dp, rows[h]] = gathered(i, h).astype(BF16)
        line_to_pair(i, h, i - 1).start()

    def settle_mid(i, h):
        total = gathered(i, h)
        part[slot(i), dp, rows[h]] = (total + line_pair_in(i, h)).astype(BF16)
        if i == 1:
            line_to_mid(1, h, 1).start()
        else:
            for c in range(2):
                far_to_mid(h, c).start()

    for n in range(6):
        i, h = n // 2 + 1, n % 2
        late.append((edge, line_to_pair(i, h, i - 1)))
        if i == 1:
            late.append((mid, line_to_mid(1, h, 1)))

    def outer(h):
        for c in range(2):
            far_in(h, c)
            strip = strip_of(h, c)
            came = line_mid[0, h, c * fine:(c + 1) * fine].astype(F32)
            part[slot(3), dp, strip] = (part[slot(3), dp, strip].astype(F32) + came).astype(BF16)
            far_to_edge(h, c).start()

    for n in range(4):
        late.append((mid, far_to_mid(n // 2, n % 2)))
        late.append((mid, far_to_edge(n // 2, n % 2)))

    load_out.wait()
    ready_two(0)
    sides_in(3, 1)
    cross_half(0, 1, gx, slot(3))
    cross_half(1, 1, gy, slot(3))
    passed_in(1, 0)
    cross_half(2, 0, gd, passed(1))
    absorb(from_passed(0))
    keep_two(0)
    ready(2, 0)
    passed_in(1, 1)
    cross_half(2, 1, gd, passed(1))
    ready_two(1)
    keep_half(2, 0)
    to_pair_passed(1, 0)
    ready(2, 1)
    keep_two(1)
    lend_all(3, 7)
    keep_half(2, 1)
    to_pair_passed(1, 1)
    keep_all(3, 5)
    to_side(2, 0, 0)
    to_side(2, 1, 1)

    @pl.when(edge)
    def _():
        to_side(2, 0, 1)
        to_side(2, 1, 0)

    keep_all(5, 7)
    to_pair_passed(0, 0)
    to_pair_passed(0, 1)
    to_corner(1, 0)
    activate(dp, 0)
    activate(dp, 1)
    lend_all(7, 9)
    to_corner(1, 1)
    lend_all(9, 11)
    keep_all(7, 9)

    @pl.when(edge)
    def _():
        settle_edge(3, 0)
        settle_edge(3, 1)

    @pl.when(mid)
    def _():
        for h in range(2):
            part[slot(3), dp, rows[h]] = gathered(3, h).astype(BF16)

    lend_all(11, 13)
    to_corner(0, 0)
    keep_all(9, 11)

    @pl.when(mid)
    def _():
        corner_add(1, 0)
        to_side(2, 1, 0)
        corner_add(1, 1)
        to_side(2, 0, 1)

    to_corner(0, 1)
    to_side(1, 0, 0)
    pl.when(edge)(functools.partial(to_side, 1, 1, 1))
    lend_all(13, 16)
    keep_all(11, 13)

    @pl.when(edge)
    def _():
        settle_edge(2, 0)
        settle_edge(2, 1)

    for role, j in ((edge, 1), (mid, 0)):

        @pl.when(role)
        def _():
            corner_add(j, 0)
            to_side(1, 1, 0)

    @pl.when(edge)
    def _():
        corner_add(1, 1)
        to_side(1, 0, 1)

    @pl.when(mid)
    def _():
        to_side(1, 1, 1)

    keep_all(13, 16)

    @pl.when(mid)
    def _():
        settle_mid(2, 0)
        settle_mid(2, 1)
        corner_add(0, 1)
        to_side(1, 0, 1)

    @pl.when(edge)
    def _():
        corner_add(0, 0)
        corner_add(0, 1)

    for h in range(2):
        to_side(0, 0, h)
        to_side(0, 1, h)

    drain(waits)

    @pl.when(edge)
    def _():
        settle_edge(1, 0)
        settle_edge(1, 1)

    @pl.when(mid)
    def _():
        settle_mid(1, 0)
        outer(0)
        settle_mid(1, 1)
        outer(1)

    for h in range(2):
        total = gathered(0, h)

        @pl.when(mid)
        def _():
            out[rows[h]] = (total + line_pair_in(0, h) + line_mid_in(1, h)).astype(BF16)

        @pl.when(edge)
        def _():
            for c in range(2):
                end_in(h, c)
            out[rows[h]] = (total + line_pair[0, h].astype(F32)).astype(BF16)

    drain(late)


def tokens_plan(tokens, routing, gate_weight, expert_in, expert_out):
    group, width = tokens.shape
    depth = lax.axis_size("expert") // 2
    experts = gate_weight.shape[1]
    model, inner = expert_in.shape[1:]
    half = group // 2
    vmem = pltpu.VMEM
    dma = pltpu.SemaphoreType.DMA
    return pl.pallas_call(
        functools.partial(whole_kernel, experts),
        out_shape=jax.ShapeDtypeStruct((group, width), BF16),
        in_specs=[pl.BlockSpec(memory_space=pl.ANY)] * 5,
        out_specs=pl.BlockSpec(memory_space=vmem),
        scratch_shapes=[
            vmem((8, width), BF16),
            vmem((experts, width), BF16),
            vmem((2, group), jnp.int32),
            vmem((4, depth, 2, group, width), BF16),
            vmem((depth, 2, 8, width), BF16),
            vmem((4, 8, width), BF16),
            vmem((model, inner), BF16),
            vmem((inner, model), BF16),
            vmem((4, group, inner), F32),
            vmem((4, 8, group), F32),
            vmem((4, group, inner), BF16),
            vmem((depth, 4, group, width), BF16),
            vmem((depth, 4, group, width), BF16),
            vmem((depth, 4, group, width), BF16),
            vmem((depth, 2, 2, half, width), BF16),
            vmem((2, 2, half, width), BF16),
            vmem((2, 2, half, width), BF16),
            vmem((3, 2, half, width), BF16),
            vmem((2, 2, half, width), BF16),
            dma((5,)),
            dma((depth, 2, 2)), dma((depth, 2, 2)),
            dma((2, 2)), dma((2, 2)),
            dma((3, 2)), dma((2, 2)), dma((3, 2)),
            dma((2, 2)), dma((2, 2)),
            dma((depth, 4)), dma((depth, 4)),
            dma((3,)), dma((3,)),
            dma((3,)), dma((2,)), dma((3,)),
            dma((depth,)), dma((depth,)),
            dma((4 * depth,)), dma((4 * depth,)),
            dma((3, 2)), dma((3, 2)), dma((3, 2)), dma((3, 2)),
            dma((depth, 2, 2)), dma((depth, 2, 2)),
            dma((2, 2)), dma((2, 2)),
            dma((2, 2)), dma((2, 2)),
            dma((3, 2)), dma((3, 2)),
            dma((2, 2)), dma((2, 2)),
            dma((4,)), dma((4,)), dma((4,)), dma((4,)),
        ],
        compiler_params=pltpu.CompilerParams(
            collective_id=0, has_side_effects=True, vmem_limit_bytes=63 * 1024 * 1024
        ),
    )(tokens, gate_weight.T, routing.T, expert_in, expert_out)


def solution(mesh):
    placed = (
        P("dp", "expert"),
        P("dp", None),
        P("expert", None),
        P("dp", None, "expert"),
        P("dp", "expert", None),
    )
    body = tokens_plan if tuple(mesh.shape.values()) == (4, 8) else slots_plan
    return jax.shard_map(
        body, mesh=mesh, in_specs=placed, out_specs=P("dp", "expert"), check_vma=False
    )
```
